16 devices in a mesh: replica: 2 (over z), data: 8 (over y, x, core).
Axes of the slice: x: 2, y: 2, z: 2, core: 2. Of those that a mesh axis runs over, the one named last changes fastest.
Arguments:
- inp_rows: bfloat16 [65536, 896], P(('replica', 'data'))
- out_grad: bfloat16 [65536, 896], P(('replica', 'data'))
- w_up: bfloat16 [2, 896, 4864], replicated
- w_down: bfloat16 [2, 4864, 896], replicated
- master_up: float32 [2, 896, 4864], P(None, 'data')
- master_down: float32 [2, 4864, 896], P(None, 'data')
- mom_up: float32 [2, 896, 4864], P(None, 'data')
- mom_down: float32 [2, 4864, 896], P(None, 'data')
- var_up: float32 [2, 896, 4864], P(None, 'data')
- var_down: float32 [2, 4864, 896], P(None, 'data')
- clip_norm: float32 [], replicated
Outputs:
- output 1: bfloat16 [2, 896, 4864], replicated
- output 2: bfloat16 [2, 4864, 896], replicated
- output 3: float32 [2, 896, 4864], P(None, 'data')
- output 4: float32 [2, 4864, 896], P(None, 'data')
- output 5: float32 [2, 896, 4864], P(None, 'data')
- output 6: float32 [2, 4864, 896], P(None, 'data')
- output 7: float32 [2, 896, 4864], P(None, 'data')
- output 8: float32 [2, 4864, 896], P(None, 'data')
- output 9: float32 [], replicated
All inputs are finite; a program needn't handle non-finite values.
Results may differ from the reference program's by a relative error of at most 0.0109783.
Values are sent between devices in bfloat16 or wider.
A program may use at most 1 GiB of HBM per device.

```python
import jax
import jax.numpy as jnp
from jax import lax

D = 896
FF = 4864
B_LOCAL = 4096
REPLICA = 2
DATA = 8
STEP = 10
DEVICES = REPLICA * DATA
ROWS = B_LOCAL * DEVICES
BETA1 = 0.9
BETA2 = 0.95
ADAM_EPS = 1e-8
LEARN_RATE = 5e-3
NORM_EPS = 1e-6
BIAS_ONE = 1.0 - BETA1 ** STEP
BIAS_TWO = 1.0 - BETA2 ** STEP


def gelu_value(pre_act):
    return pre_act * (0.5 + 0.5 * lax.erf(pre_act * 0.7071067811865476))


def gelu_slope(pre_act):
    return 0.5 + 0.5 * lax.erf(pre_act * 0.7071067811865476) + pre_act * jnp.exp(-0.5 * pre_act * pre_act) * 0.3989422804014327


def matmul(left_mat, right_mat):
    return jnp.dot(left_mat, right_mat, preferred_element_type=jnp.float32)


def device_grads(inp_rows, out_grad, w_up, w_down):
    pre_one = matmul(inp_rows, w_up[0]).astype(jnp.bfloat16)
    act_one = gelu_value(pre_one.astype(jnp.float32)).astype(jnp.bfloat16)
    mid_rows = matmul(act_one, w_down[0]).astype(jnp.bfloat16)
    pre_two = matmul(mid_rows, w_up[1]).astype(jnp.bfloat16)
    act_two = gelu_value(pre_two.astype(jnp.float32)).astype(jnp.bfloat16)
    grad_down2 = matmul(act_two.T, out_grad)
    dact_two = matmul(out_grad, w_down[1].T).astype(jnp.bfloat16)
    dpre_two = (dact_two.astype(jnp.float32) * gelu_slope(pre_two.astype(jnp.float32))).astype(jnp.bfloat16)
    grad_up2 = matmul(mid_rows.T, dpre_two)
    dmid_rows = matmul(dpre_two, w_up[1].T).astype(jnp.bfloat16)
    grad_down1 = matmul(act_one.T, dmid_rows)
    dact_one = matmul(dmid_rows, w_down[0].T).astype(jnp.bfloat16)
    dpre_one = (dact_one.astype(jnp.float32) * gelu_slope(pre_one.astype(jnp.float32))).astype(jnp.bfloat16)
    grad_up1 = matmul(inp_rows.T, dpre_one)
    return jnp.stack([grad_up1, grad_up2]), jnp.stack([grad_down1, grad_down2])


def mean_grads(inp_rows, out_grad, w_up, w_down):
    inp_blocks = inp_rows.reshape(DEVICES, B_LOCAL, D)
    grad_blocks = out_grad.reshape(DEVICES, B_LOCAL, D)

    def scan_step(carry_sums, block_pair):
        up_part, down_part = device_grads(block_pair[0], block_pair[1], w_up, w_down)
        return (carry_sums[0] + up_part, carry_sums[1] + down_part), None

    zero_carry = (jnp.zeros((2, D, FF), jnp.float32), jnp.zeros((2, FF, D), jnp.float32))
    totals, unused = lax.scan(scan_step, zero_carry, (inp_blocks, grad_blocks))
    return totals[0] / DEVICES, totals[1] / DEVICES


def adam_update(grad_vals, master_vals, mom_vals, var_vals, clip_scale):
    new_mom = BETA1 * mom_vals + (1.0 - BETA1) * clip_scale * grad_vals
    new_var = BETA2 * var_vals + (1.0 - BETA2) * (clip_scale * clip_scale) * (grad_vals * grad_vals)
    new_master = master_vals - LEARN_RATE * (new_mom / BIAS_ONE) / (jnp.sqrt(new_var / BIAS_TWO) + ADAM_EPS)
    return new_master, new_mom, new_var


def setup_inputs(seed: int = 0) -> dict:
    keys = jax.random.split(jax.random.key(seed), 9)
    inp_rows = jax.random.normal(keys[0], (ROWS, D), jnp.float32).astype(jnp.bfloat16)
    out_grad = jax.random.normal(keys[1], (ROWS, D), jnp.float32).astype(jnp.bfloat16)
    down_gain = jnp.array([1.6, 1.4], jnp.float32).reshape(2, 1, 1)
    master_up = jax.random.normal(keys[2], (2, D, FF), jnp.float32) * D ** -0.5
    master_down = jax.random.normal(keys[3], (2, FF, D), jnp.float32) * down_gain * FF ** -0.5
    w_up = master_up.astype(jnp.bfloat16)
    w_down = master_down.astype(jnp.bfloat16)
    grad_up, grad_down = mean_grads(inp_rows, out_grad, w_up, w_down)
    true_norm = jnp.sqrt(jnp.sum(grad_up * grad_up) + jnp.sum(grad_down * grad_down))
    clip_frac = jax.random.uniform(keys[4], (), jnp.float32, minval=0.3, maxval=0.7)
    up_size = clip_frac * jnp.sqrt(jnp.mean(grad_up * grad_up, axis=(1, 2), keepdims=True))
    down_size = clip_frac * jnp.sqrt(jnp.mean(grad_down * grad_down, axis=(1, 2), keepdims=True))
    mom_up = (1.0 - BETA1) * up_size * jax.random.normal(keys[5], (2, D, FF), jnp.float32)
    mom_down = (1.0 - BETA1) * down_size * jax.random.normal(keys[6], (2, FF, D), jnp.float32)
    var_up = (1.0 - BETA2) * up_size * up_size * jax.random.uniform(keys[7], (2, D, FF), jnp.float32, minval=0.25, maxval=2.0)
    var_down = (1.0 - BETA2) * down_size * down_size * jax.random.uniform(keys[8], (2, FF, D), jnp.float32, minval=0.25, maxval=2.0)
    return {'inp_rows': inp_rows, 'out_grad': out_grad, 'w_up': w_up, 'w_down': w_down, 'master_up': master_up, 'master_down': master_down, 'mom_up': mom_up, 'mom_down': mom_down, 'var_up': var_up, 'var_down': var_down, 'clip_norm': clip_frac * true_norm}


def reference(inp_rows, out_grad, w_up, w_down, master_up, master_down, mom_up, mom_down, var_up, var_down, clip_norm):
    grad_up, grad_down = mean_grads(inp_rows, out_grad, w_up, w_down)
    grad_norm = jnp.sqrt(jnp.sum(grad_up * grad_up) + jnp.sum(grad_down * grad_down))
    clip_scale = jnp.minimum(1.0, clip_norm / (grad_norm + NORM_EPS))
    master_up_new, mom_up_new, var_up_new = adam_update(grad_up, master_up, mom_up, var_up, clip_scale)
    master_down_new, mom_down_new, var_down_new = adam_update(grad_down, master_down, mom_down, var_down, clip_scale)
    return (master_up_new.astype(jnp.bfloat16), master_down_new.astype(jnp.bfloat16), master_up_new, master_down_new, mom_up_new, mom_down_new, var_up_new, var_down_new, grad_norm)
```

```python
import functools

import jax
import jax.numpy as jnp
from jax import lax
from jax.experimental import pallas as pl
from jax.experimental.pallas import tpu as pltpu
from jax.sharding import PartitionSpec as P

BETA1 = 0.9
BETA2 = 0.95
ADAM_EPS = 1e-8
LEARN_RATE = 5e-3
NORM_EPS = 1e-6
STEP = 10
BIAS_ONE = 1.0 - BETA1 ** STEP
BIAS_TWO = 1.0 - BETA2 ** STEP

F32 = jnp.float32
BF16 = jnp.bfloat16
ROWS = 4096
D = 896
FF = 4864
TILE = 256
NT = FF // TILE
OWN = 8
PIECE = TILE // OWN
RM = 1024
VMEM_LIMIT = 67_043_328


def gelu_value(pre_act):
    return pre_act * (0.5 + 0.5 * lax.erf(pre_act * 0.7071067811865476))


def gelu_both(pre_act):
    cdf = 0.5 + 0.5 * lax.erf(pre_act * 0.7071067811865476)
    return pre_act * cdf, cdf + pre_act * jnp.exp(-0.5 * pre_act * pre_act) * 0.3989422804014327


def mm(left, right):
    return jnp.dot(left, right, preferred_element_type=F32)


def mm_nt(left, right):
    return lax.dot_general(left, right, (((1,), (1,)), ((), ())), preferred_element_type=F32)


def permute_kernel(w_ref, out_ref):
    for t in range(NT):
        out_ref[:, t * TILE:(t + 1) * TILE] = jnp.concatenate(
            [w_ref[:, d * (FF // OWN) + t * PIECE:d * (FF // OWN) + (t + 1) * PIECE] for d in range(OWN)], axis=1)


def permute_columns(w_up):
    rows = 128
    flat = w_up.reshape(2 * D, FF)
    out = pl.pallas_call(
        permute_kernel,
        grid=(2 * D // rows,),
        in_specs=[pl.BlockSpec((rows, FF), lambda i: (i, 0))],
        out_specs=pl.BlockSpec((rows, FF), lambda i: (i, 0)),
        out_shape=jax.ShapeDtypeStruct((2 * D, FF), w_up.dtype),
        name="permute_columns",
    )(flat)
    return out.reshape(2, D, FF)


def forward_kernel(x_ref, wu_ref, wd_ref, z_ref, h_ref, acc):
    t = pl.program_id(0)

    @pl.when(t == 0)
    def _():
        acc[...] = jnp.zeros_like(acc)

    wd = wd_ref[0, :, 0].reshape(TILE, D)

    def body(r, carry):
        rows = pl.ds(pl.multiple_of(r * RM, RM), RM)
        z = mm(x_ref[rows, :], wu_ref[0]).astype(BF16)
        z_ref[0, rows, :] = z
        u = gelu_value(z.astype(F32)).astype(BF16)
        acc[rows, :] += mm(u, wd)
        return carry

    lax.fori_loop(0, ROWS // RM, body, 0)

    @pl.when(t == NT - 1)
    def _():
        h_ref[...] = acc[...].astype(BF16)


def forward(x, w_upp, w_down5):
    return pl.pallas_call(
        forward_kernel,
        grid=(NT,),
        in_specs=[
            pl.BlockSpec((ROWS, D), lambda t: (0, 0), pipeline_mode=pl.Buffered(1)),
            pl.BlockSpec((1, D, TILE), lambda t: (0, 0, t)),
            pl.BlockSpec((1, OWN, 1, PIECE, D), lambda t: (0, 0, t, 0, 0)),
        ],
        out_specs=[
            pl.BlockSpec((1, ROWS, TILE), lambda t: (t, 0, 0)),
            pl.BlockSpec((ROWS, D), lambda t: (0, 0), pipeline_mode=pl.Buffered(1)),
        ],
        out_shape=[jax.ShapeDtypeStruct((NT, ROWS, TILE), BF16), jax.ShapeDtypeStruct((ROWS, D), BF16)],
        scratch_shapes=[pltpu.VMEM((ROWS, D), F32)],
        compiler_params=pltpu.CompilerParams(vmem_limit_bytes=VMEM_LIMIT),
        name="forward",
    )(x, w_upp, w_down5)


def upper_kernel(h_hbm, ht_hbm, dy_hbm, dyt_hbm, wu_ref, wd_ref, gd_ref, gu_ref, dh_hbm,
                 h, ht, dy, dyt, acc, u_s, d_s, sems):
    t = pl.program_id(0)
    loads = [pltpu.make_async_copy(s, v, sems.at[i]) for i, (s, v) in
             enumerate([(h_hbm, h), (dy_hbm, dy), (dyt_hbm, dyt), (ht_hbm, ht)])]

    @pl.when(t == 0)
    def _():
        for copy in loads:
            copy.start()
        acc[...] = jnp.zeros_like(acc)
        loads[0].wait()
        loads[1].wait()

    wu = wu_ref[0]
    wd = wd_ref[0, :, 0].reshape(TILE, D)

    def body(r, carry):
        rows = pl.ds(pl.multiple_of(r * RM, RM), RM)
        z = mm(h[rows, :], wu).astype(BF16).astype(F32)
        e = mm_nt(dy[rows, :], wd).astype(BF16).astype(F32)
        u, slope = gelu_both(z)
        u_s[rows, :] = u.astype(BF16)
        dz = (e * slope).astype(BF16)
        d_s[rows, :] = dz
        acc[rows, :] += mm_nt(dz, wu)
        return carry

    lax.fori_loop(0, ROWS // RM, body, 0)

    @pl.when(t == 0)
    def _():
        loads[2].wait()
        loads[3].wait()

    gd_ref[:, 0] = mm(dyt[...], u_s[...]).T.reshape(OWN, PIECE, D)
    gu_ref[...] = mm(ht[...], d_s[...])

    @pl.when(t == NT - 1)
    def _():
        h[...] = acc[...].astype(BF16)
        out = pltpu.make_async_copy(h, dh_hbm, sems.at[0])
        out.start()
        out.wait()


def upper(h, ht, dy, dyt, w_upp, w_down5):
    anyspec = pl.BlockSpec(memory_space=pl.ANY)
    return pl.pallas_call(
        upper_kernel,
        grid=(NT,),
        in_specs=[anyspec] * 4 + [
            pl.BlockSpec((1, D, TILE), lambda t: (1, 0, t)),
            pl.BlockSpec((1, OWN, 1, PIECE, D), lambda t: (1, 0, t, 0, 0)),
        ],
        out_specs=[
            pl.BlockSpec((OWN, 1, PIECE, D), lambda t: (0, t, 0, 0)),
            pl.BlockSpec((D, TILE), lambda t: (0, t)),
            anyspec,
        ],
        out_shape=[jax.ShapeDtypeStruct((OWN, NT, PIECE, D), F32), jax.ShapeDtypeStruct((D, FF), F32),
                   jax.ShapeDtypeStruct((ROWS, D), BF16)],
        scratch_shapes=[pltpu.VMEM((ROWS, D), BF16), pltpu.VMEM((D, ROWS), BF16),
                        pltpu.VMEM((ROWS, D), BF16), pltpu.VMEM((D, ROWS), BF16),
                        pltpu.VMEM((ROWS, D), F32), pltpu.VMEM((ROWS, TILE), BF16), pltpu.VMEM((ROWS, TILE), BF16),
                        pltpu.SemaphoreType.DMA((4,))],
        compiler_params=pltpu.CompilerParams(vmem_limit_bytes=VMEM_LIMIT),
        name="upper",
    )(h, ht, dy, dyt, w_upp, w_down5)


def lower_kernel(dh_hbm, dht_hbm, xt_hbm, z_ref, wd_ref, gd_ref, gu_ref,
                 dh, dht, xt, u_s, d_s, sems):
    t = pl.program_id(0)
    loads = [pltpu.make_async_copy(s, v, sems.at[i]) for i, (s, v) in
             enumerate([(dh_hbm, dh), (dht_hbm, dht), (xt_hbm, xt)])]

    @pl.when(t == 0)
    def _():
        for copy in loads:
            copy.start()
        loads[0].wait()

    wd = wd_ref[0, :, 0].reshape(TILE, D)

    def body(r, carry):
        rows = pl.ds(pl.multiple_of(r * RM, RM), RM)
        z = z_ref[0, rows, :].astype(F32)
        e = mm_nt(dh[rows, :], wd).astype(BF16).astype(F32)
        u, slope = gelu_both(z)
        u_s[rows, :] = u.astype(BF16)
        d_s[rows, :] = (e * slope).astype(BF16)
        return carry

    lax.fori_loop(0, ROWS // RM, body, 0)

    @pl.when(t == 0)
    def _():
        loads[1].wait()
        loads[2].wait()

    gd_ref[:, 0] = mm(dht[...], u_s[...]).T.reshape(OWN, PIECE, D)
    gu_ref[...] = mm(xt[...], d_s[...])


def lower(dh, dht, xt, z, w_down5):
    anyspec = pl.BlockSpec(memory_space=pl.ANY)
    return pl.pallas_call(
        lower_kernel,
        grid=(NT,),
        in_specs=[anyspec] * 3 + [
            pl.BlockSpec((1, ROWS, TILE), lambda t: (t, 0, 0)),
            pl.BlockSpec((1, OWN, 1, PIECE, D), lambda t: (0, 0, t, 0, 0)),
        ],
        out_specs=[
            pl.BlockSpec((OWN, 1, PIECE, D), lambda t: (0, t, 0, 0)),
            pl.BlockSpec((D, TILE), lambda t: (0, t)),
        ],
        out_shape=[jax.ShapeDtypeStruct((OWN, NT, PIECE, D), F32), jax.ShapeDtypeStruct((D, FF), F32)],
        scratch_shapes=[pltpu.VMEM((ROWS, D), BF16), pltpu.VMEM((D, ROWS), BF16), pltpu.VMEM((D, ROWS), BF16),
                        pltpu.VMEM((ROWS, TILE), BF16), pltpu.VMEM((ROWS, TILE), BF16),
                        pltpu.SemaphoreType.DMA((3,))],
        compiler_params=pltpu.CompilerParams(vmem_limit_bytes=VMEM_LIMIT),
        name="lower",
    )(dh, dht, xt, z, w_down5)


def adam_update(grad_vals, master_vals, mom_vals, var_vals, clip_scale):
    new_mom = BETA1 * mom_vals + (1.0 - BETA1) * clip_scale * grad_vals
    new_var = BETA2 * var_vals + (1.0 - BETA2) * (clip_scale * clip_scale) * (grad_vals * grad_vals)
    new_master = master_vals - LEARN_RATE * (new_mom / BIAS_ONE) / (jnp.sqrt(new_var / BIAS_TWO) + ADAM_EPS)
    return new_master, new_mom, new_var


def unpermute(shard):
    rows = shard.shape[0]
    return shard.reshape(rows, NT, OWN, PIECE).transpose(0, 2, 1, 3).reshape(rows, FF)


def solution(mesh):
    total_devices = mesh.shape['replica'] * mesh.shape['data']
    batch_spec = P(('replica', 'data'), None)
    whole_spec = P()
    shard_spec = P(None, 'data', None)

    def device_step(inp_rows, out_grad, w_up, w_down, master_up, master_down, mom_up, mom_down, var_up, var_down, clip_norm):
        w_upp = permute_columns(w_up)
        w_down5 = w_down.reshape(2, OWN, NT, PIECE, D)
        pre_one, mid_rows = forward(inp_rows, w_upp, w_down5)
        grad_down2, grad_up2, dmid_rows = upper(mid_rows, mid_rows.T, out_grad, out_grad.T, w_upp, w_down5)
        grad_down1, grad_up1 = lower(dmid_rows, dmid_rows.T, inp_rows.T, pre_one, w_down5)
        grad_down2 = grad_down2.reshape(FF, D)
        grad_down1 = grad_down1.reshape(FF, D)
        shard_down2 = lax.psum_scatter(grad_down2, 'data', scatter_dimension=0, tiled=True)
        shard_up2 = lax.psum_scatter(grad_up2, 'data', scatter_dimension=0, tiled=True)
        shard_down1 = lax.psum_scatter(grad_down1, 'data', scatter_dimension=0, tiled=True)
        shard_up1 = lax.psum_scatter(grad_up1, 'data', scatter_dimension=0, tiled=True)
        shard_up1 = unpermute(shard_up1)
        shard_up2 = unpermute(shard_up2)
        grad_up = lax.psum(jnp.stack([shard_up1, shard_up2]), 'replica') / total_devices
        grad_down = lax.psum(jnp.stack([shard_down1, shard_down2]), 'replica') / total_devices
        local_sq = jnp.sum(grad_up * grad_up) + jnp.sum(grad_down * grad_down)
        grad_norm = jnp.sqrt(lax.psum(local_sq, 'data'))
        clip_scale = jnp.minimum(1.0, clip_norm / (grad_norm + NORM_EPS))
        master_up_new, mom_up_new, var_up_new = adam_update(grad_up, master_up, mom_up, var_up, clip_scale)
        master_down_new, mom_down_new, var_down_new = adam_update(grad_down, master_down, mom_down, var_down, clip_scale)
        w_up_new = lax.all_gather(master_up_new.astype(jnp.bfloat16), 'data', axis=1, tiled=True)
        w_down_new = lax.all_gather(master_down_new.astype(jnp.bfloat16), 'data', axis=1, tiled=True)
        return (w_up_new, w_down_new, master_up_new, master_down_new, mom_up_new, mom_down_new, var_up_new, var_down_new, grad_norm)

    return jax.shard_map(device_step, mesh=mesh, in_specs=(batch_spec, batch_spec, whole_spec, whole_spec, shard_spec, shard_spec, shard_spec, shard_spec, shard_spec, shard_spec, whole_spec), out_specs=(whole_spec, whole_spec, shard_spec, shard_spec, shard_spec, shard_spec, shard_spec, shard_spec, whole_spec), check_vma=False)
```

```python
import functools

import jax
import jax.numpy as jnp
from jax import lax
from jax.experimental import pallas as pl
from jax.experimental.pallas import tpu as pltpu
from jax.sharding import PartitionSpec as P

BETA1 = 0.9
BETA2 = 0.95
ADAM_EPS = 1e-8
LEARN_RATE = 5e-3
NORM_EPS = 1e-6
STEP = 10
BIAS_ONE = 1.0 - BETA1 ** STEP
BIAS_TWO = 1.0 - BETA2 ** STEP

F32 = jnp.float32
BF16 = jnp.bfloat16
ROWS = 4096
D = 896
FF = 4864
TILE = 256
NT = FF // TILE
OWN = 8
PIECE = TILE // OWN
RM = 512
NB = ROWS // RM
VMEM_LIMIT = 67_043_328


def gelu_value(pre_act):
    return pre_act * (0.5 + 0.5 * lax.erf(pre_act * 0.7071067811865476))


def gelu_both(pre_act):
    cdf = 0.5 + 0.5 * lax.erf(pre_act * 0.7071067811865476)
    return pre_act * cdf, cdf + pre_act * jnp.exp(-0.5 * pre_act * pre_act) * 0.3989422804014327


def mm(left, right):
    return jnp.dot(left, right, preferred_element_type=F32)


def mm_nt(left, right):
    return lax.dot_general(left, right, (((1,), (1,)), ((), ())), preferred_element_type=F32)


MESH = pl.DeviceIdType.MESH
LAG = 4
GRID = NT + LAG


def coordinates():
    d = lax.axis_index('data')
    z = lax.axis_index('replica')
    c = lax.rem(d, 2)
    x = lax.rem(lax.div(d, 2), 2)
    y = lax.div(d, 4)
    peers = {
        'c': {'data': d + 1 - 2 * c},
        'x': {'data': d + 2 - 4 * x},
        'y': {'data': d + 4 - 8 * y},
        'z': {'replica': 1 - z},
    }
    return d, c, x, y, z, peers


def neighbour_barrier(peers):
    barrier = pltpu.get_barrier_semaphore()
    for peer in peers:
        pl.semaphore_signal(barrier, inc=1, device_id=peer, device_id_type=MESH)
    pl.semaphore_wait(barrier, len(peers))


def grad_scratch(rows, cols):
    return [pltpu.VMEM((2, 2, 2, rows, cols), F32),
            pltpu.VMEM((2, 2, 2, rows, cols), F32),
            pltpu.VMEM((2, 2, rows, cols), F32),
            pltpu.VMEM((2, 2, rows, cols), F32),
            pltpu.VMEM((2, rows, cols), F32),
            pltpu.VMEM((2, rows, cols), F32),
            pltpu.VMEM((rows, cols), F32),
            pltpu.VMEM((2, rows, cols), F32),
            pltpu.SemaphoreType.DMA((4, 2)),
            pltpu.SemaphoreType.DMA((4, 2))]


class Reducer:
    def __init__(self, scratch, x_first, t):
        (self.tile, self.in_core, self.chip, self.in_one, self.two, self.in_two, self.four, self.in_rep,
         self.send, self.recv) = scratch
        self.x_first = x_first
        self.t = t
        _, self.c, self.x, self.y, _, self.peers = coordinates()

    def copy(self, stage, tile_index):
        slot = lax.rem(tile_index + 2, 2)
        first, second = ('x', 'y') if self.x_first else ('y', 'x')
        if stage == 0:
            src, dst, peer = self.tile.at[:, :, 1 - self.c], self.in_core.at[slot], 'c'
        elif stage == 1:
            src = self.chip.at[:, 1 - self.x] if self.x_first else self.chip.at[1 - self.y]
            dst, peer = self.in_one.at[slot], first
        elif stage == 2:
            src = self.two.at[1 - self.y] if self.x_first else self.two.at[1 - self.x]
            dst, peer = self.in_two.at[slot], second
        else:
            src, dst, peer = self.four, self.in_rep.at[slot], 'z'
        return pltpu.make_async_remote_copy(
            src_ref=src, dst_ref=dst, send_sem=self.send.at[stage, slot], recv_sem=self.recv.at[stage, slot],
            device_id=self.peers[peer], device_id_type=MESH)

    def start(self):
        self.copy(0, self.t).start()

    def progress(self, out_ref, sq_ref):
        t = self.t

        @pl.when(t >= 4)
        def _():
            self.copy(3, t - 4).wait()
            total = self.four[...] + self.in_rep[lax.rem(t, 2)]
            out_ref[0] = total
            sq_ref[...] += jnp.sum(total * total, axis=0, keepdims=True)

        @pl.when((t >= 3) & (t < NT + 3))
        def _():
            self.copy(2, t - 3).wait()
            mine = self.two[self.y] if self.x_first else self.two[self.x]
            self.four[...] = mine + self.in_two[lax.rem(t + 1, 2)]
            self.copy(3, t - 3).start()

        @pl.when((t >= 2) & (t < NT + 2))
        def _():
            self.copy(1, t - 2).wait()
            mine = self.chip[:, self.x] if self.x_first else self.chip[self.y]
            self.two[...] = mine + self.in_one[lax.rem(t, 2)]
            self.copy(2, t - 2).start()

        @pl.when((t >= 1) & (t < NT + 1))
        def _():
            self.copy(0, t - 1).wait()
            self.chip[...] = self.tile[:, :, self.c] + self.in_core[lax.rem(t + 1, 2)]
            self.copy(1, t - 1).start()


def permute_kernel(w_ref, out_ref):
    for t in range(NT):
        out_ref[:, t * TILE:(t + 1) * TILE] = jnp.concatenate(
            [w_ref[:, d * (FF // OWN) + t * PIECE:d * (FF // OWN) + (t + 1) * PIECE] for d in range(OWN)], axis=1)


def permute_columns(w_up):
    rows = 128
    flat = w_up.reshape(2 * D, FF)
    out = pl.pallas_call(
        permute_kernel,
        grid=(2 * D // rows,),
        in_specs=[pl.BlockSpec((rows, FF), lambda i: (i, 0))],
        out_specs=pl.BlockSpec((rows, FF), lambda i: (i, 0)),
        out_shape=jax.ShapeDtypeStruct((2 * D, FF), w_up.dtype),
        name="permute_columns",
    )(flat)
    return out.reshape(2, D, FF)


def forward_kernel(x_ref, wu_ref, wd_ref, z_ref, h_ref, acc):
    t = pl.program_id(0)

    @pl.when(t == 0)
    def _():
        acc[...] = jnp.zeros_like(acc)

    wd = wd_ref[0, :, 0].reshape(TILE, D)

    for r in range(NB + 1):
        if r < NB:
            rows = pl.ds(r * RM, RM)
            z_ref[0, rows, :] = mm(x_ref[rows, :], wu_ref[0]).astype(BF16)
        if r > 0:
            rows = pl.ds((r - 1) * RM, RM)
            u = gelu_value(z_ref[0, rows, :].astype(F32)).astype(BF16)
            acc[rows, :] += mm(u, wd)

    @pl.when(t == NT - 1)
    def _():
        h_ref[...] = acc[...].astype(BF16)


def forward(x, w_upp, w_down5):
    return pl.pallas_call(
        forward_kernel,
        grid=(NT,),
        in_specs=[
            pl.BlockSpec((ROWS, D), lambda t: (0, 0), pipeline_mode=pl.Buffered(1)),
            pl.BlockSpec((1, D, TILE), lambda t: (0, 0, t)),
            pl.BlockSpec((1, OWN, 1, PIECE, D), lambda t: (0, 0, t, 0, 0)),
        ],
        out_specs=[
            pl.BlockSpec((1, ROWS, TILE), lambda t: (t, 0, 0)),
            pl.BlockSpec((ROWS, D), lambda t: (0, 0), pipeline_mode=pl.Buffered(1)),
        ],
        out_shape=[jax.ShapeDtypeStruct((NT, ROWS, TILE), BF16), jax.ShapeDtypeStruct((ROWS, D), BF16)],
        scratch_shapes=[pltpu.VMEM((ROWS, D), F32)],
        compiler_params=pltpu.CompilerParams(vmem_limit_bytes=VMEM_LIMIT),
        name="forward",
    )(x, w_upp, w_down5)


def upper_kernel(h_hbm, ht_hbm, dy_hbm, dyt_hbm, wu_ref, wd_ref, gd_ref, gu_ref, sqd_ref, squ_ref, dh_hbm, dht_hbm,
                 h, ht, dy, dyt, acc, u_s, d_s, sems, *grads):
    t = pl.program_id(0)
    loads = [pltpu.make_async_copy(s, v, sems.at[i]) for i, (s, v) in
             enumerate([(h_hbm, h), (dy_hbm, dy), (dyt_hbm, dyt), (ht_hbm, ht)])]
    stores = [pltpu.make_async_copy(h, dh_hbm, sems.at[0]), pltpu.make_async_copy(ht, dht_hbm, sems.at[1])]
    down = Reducer(grads[:10], True, t)
    up = Reducer(grads[10:], False, t)

    @pl.when(t == 0)
    def _():
        for copy in loads:
            copy.start()
        neighbour_barrier([down.peers[k] for k in 'cxyz'])
        acc[...] = jnp.zeros_like(acc)
        sqd_ref[...] = jnp.zeros_like(sqd_ref)
        squ_ref[...] = jnp.zeros_like(squ_ref)
        loads[0].wait()
        loads[1].wait()

    def rows_of(first, last):
        wu = wu_ref[0]
        wd = wd_ref[0, :, 0].reshape(TILE, D)
        for r in range(first, last):
            if r < NB:
                rows = pl.ds(r * RM, RM)
                u_s[rows, :] = mm(h[rows, :], wu).astype(BF16)
                d_s[rows, :] = mm_nt(dy[rows, :], wd).astype(BF16)
            if r > 0:
                rows = pl.ds((r - 1) * RM, RM)
                u, slope = gelu_both(u_s[rows, :].astype(F32))
                dz = (d_s[rows, :].astype(F32) * slope).astype(BF16)
                u_s[rows, :] = u.astype(BF16)
                d_s[rows, :] = dz
                acc[rows, :] += mm_nt(dz, wu)

    @pl.when(t < NT)
    def _():
        rows_of(0, NB // 2)

    down.progress(gd_ref, sqd_ref)

    @pl.when(t < NT)
    def _():
        rows_of(NB // 2, NB + 1)

    up.progress(gu_ref, squ_ref)

    @pl.when(t == 0)
    def _():
        loads[2].wait()
        loads[3].wait()

    @pl.when(t < NT)
    def _():
        down.tile[...] = mm(dyt[...], u_s[...]).T.reshape(2, 2, 2, PIECE, D)
        up.tile[...] = mm(ht[...], d_s[...]).reshape(2, 2, 2, D // OWN, TILE)
        down.start()
        up.start()

    @pl.when(t == NT - 1)
    def _():
        h[...] = acc[...].astype(BF16)
        stores[0].start()

    @pl.when(t == NT)
    def _():
        ht[...] = h[...].T
        stores[1].start()

    @pl.when(t == GRID - 1)
    def _():
        stores[0].wait()
        stores[1].wait()


def final_tile(t):
    return jnp.clip(t - LAG, 0, NT - 1)


def this_tile(t):
    return jnp.minimum(t, NT - 1)


GRAD_SPECS = [
    pl.BlockSpec((1, PIECE, D), lambda t: (final_tile(t), 0, 0)),
    pl.BlockSpec((1, D // OWN, TILE), lambda t: (final_tile(t), 0, 0)),
    pl.BlockSpec((1, D), lambda t: (0, 0)),
    pl.BlockSpec((1, TILE), lambda t: (0, 0)),
]
GRAD_SHAPES = [
    jax.ShapeDtypeStruct((NT, PIECE, D), F32),
    jax.ShapeDtypeStruct((NT, D // OWN, TILE), F32),
    jax.ShapeDtypeStruct((1, D), F32),
    jax.ShapeDtypeStruct((1, TILE), F32),
]


def upper(h, ht, dy, dyt, w_upp, w_down5):
    anyspec = pl.BlockSpec(memory_space=pl.ANY)
    return pl.pallas_call(
        upper_kernel,
        grid=(GRID,),
        in_specs=[anyspec] * 4 + [
            pl.BlockSpec((1, D, TILE), lambda t: (1, 0, this_tile(t))),
            pl.BlockSpec((1, OWN, 1, PIECE, D), lambda t: (1, 0, this_tile(t), 0, 0)),
        ],
        out_specs=GRAD_SPECS + [anyspec, anyspec],
        out_shape=GRAD_SHAPES + [jax.ShapeDtypeStruct((ROWS, D), BF16), jax.ShapeDtypeStruct((D, ROWS), BF16)],
        scratch_shapes=[pltpu.VMEM((ROWS, D), BF16), pltpu.VMEM((D, ROWS), BF16),
                        pltpu.VMEM((ROWS, D), BF16), pltpu.VMEM((D, ROWS), BF16),
                        pltpu.VMEM((ROWS, D), F32), pltpu.VMEM((ROWS, TILE), BF16), pltpu.VMEM((ROWS, TILE), BF16),
                        pltpu.SemaphoreType.DMA((4,))] + grad_scratch(PIECE, D) + grad_scratch(D // OWN, TILE),
        compiler_params=pltpu.CompilerParams(vmem_limit_bytes=VMEM_LIMIT, collective_id=0, has_side_effects=True),
        name="upper",
    )(h, ht, dy, dyt, w_upp, w_down5)


def lower_kernel(sqd_in, squ_in, dh_hbm, dht_hbm, xt_hbm, z_ref, wd_ref, gd_ref, gu_ref, sqd_ref, squ_ref, norm_ref,
                 dh, dht, xt, u_s, d_s, sems, sq_mine, sq_all, sq_send, sq_recv, *grads):
    t = pl.program_id(0)
    loads = [pltpu.make_async_copy(s, v, sems.at[i]) for i, (s, v) in
             enumerate([(dh_hbm, dh), (dht_hbm, dht), (xt_hbm, xt)])]
    down = Reducer(grads[:10], True, t)
    up = Reducer(grads[10:], False, t)
    me = lax.axis_index('data')
    others = [{'data': lax.rem(me + k, OWN)} for k in range(1, OWN)]

    @pl.when(t == 0)
    def _():
        for copy in loads:
            copy.start()
        neighbour_barrier(others + [down.peers['z']])
        sqd_ref[...] = sqd_in[...]
        squ_ref[...] = squ_in[...]
        loads[0].wait()

    def rows_of(first, last):
        wd = wd_ref[0, :, 0].reshape(TILE, D)
        for r in range(first, last):
            if r < NB:
                rows = pl.ds(r * RM, RM)
                d_s[rows, :] = mm_nt(dh[rows, :], wd).astype(BF16)
            if r > 0:
                rows = pl.ds((r - 1) * RM, RM)
                u, slope = gelu_both(z_ref[0, rows, :].astype(F32))
                u_s[rows, :] = u.astype(BF16)
                d_s[rows, :] = (d_s[rows, :].astype(F32) * slope).astype(BF16)

    @pl.when(t < NT)
    def _():
        rows_of(0, NB // 2)

    down.progress(gd_ref, sqd_ref)

    @pl.when(t < NT)
    def _():
        rows_of(NB // 2, NB + 1)

    up.progress(gu_ref, squ_ref)

    @pl.when(t == 0)
    def _():
        loads[1].wait()
        loads[2].wait()

    @pl.when(t < NT)
    def _():
        down.tile[...] = mm(dht[...], u_s[...]).T.reshape(2, 2, 2, PIECE, D)
        up.tile[...] = mm(xt[...], d_s[...]).reshape(2, 2, 2, D // OWN, TILE)
        down.start()
        up.start()

    @pl.when(t == GRID - 1)
    def _():
        part = jnp.sum(sqd_ref[...], axis=1, keepdims=True) + jnp.sum(squ_ref[...], axis=1, keepdims=True)
        sq_mine[...] = jnp.broadcast_to(part, sq_mine.shape)
        sq_all[me] = sq_mine[...]
        copies = [pltpu.make_async_remote_copy(
            src_ref=sq_mine, dst_ref=sq_all.at[me], send_sem=sq_send.at[k], recv_sem=sq_recv.at[k],
            device_id=others[k], device_id_type=MESH) for k in range(OWN - 1)]
        for copy in copies:
            copy.start()
        for copy in copies:
            copy.wait()
        total = sq_all[0]
        for k in range(1, OWN):
            total = total + sq_all[k]
        norm_ref[...] = total


def lower(sqd, squ, dh, dht, xt, z, w_down5):
    anyspec = pl.BlockSpec(memory_space=pl.ANY)
    return pl.pallas_call(
        lower_kernel,
        grid=(GRID,),
        in_specs=GRAD_SPECS[2:] + [anyspec] * 3 + [
            pl.BlockSpec((1, ROWS, TILE), lambda t: (this_tile(t), 0, 0)),
            pl.BlockSpec((1, OWN, 1, PIECE, D), lambda t: (0, 0, this_tile(t), 0, 0)),
        ],
        out_specs=GRAD_SPECS + [pl.BlockSpec((8, 128), lambda t: (0, 0))],
        out_shape=GRAD_SHAPES + [jax.ShapeDtypeStruct((8, 128), F32)],
        scratch_shapes=[pltpu.VMEM((ROWS, D), BF16), pltpu.VMEM((D, ROWS), BF16), pltpu.VMEM((D, ROWS), BF16),
                        pltpu.VMEM((ROWS, TILE), BF16), pltpu.VMEM((ROWS, TILE), BF16),
                        pltpu.SemaphoreType.DMA((3,)),
                        pltpu.VMEM((8, 128), F32), pltpu.VMEM((OWN, 8, 128), F32),
                        pltpu.SemaphoreType.DMA((OWN - 1,)), pltpu.SemaphoreType.DMA((OWN - 1,))]
        + grad_scratch(PIECE, D) + grad_scratch(D // OWN, TILE),
        compiler_params=pltpu.CompilerParams(vmem_limit_bytes=VMEM_LIMIT, collective_id=1, has_side_effects=True),
        name="lower",
    )(sqd, squ, dh, dht, xt, z, w_down5)


def adam_update(grad_vals, master_vals, mom_vals, var_vals, clip_scale):
    new_mom = BETA1 * mom_vals + (1.0 - BETA1) * clip_scale * grad_vals
    new_var = BETA2 * var_vals + (1.0 - BETA2) * (clip_scale * clip_scale) * (grad_vals * grad_vals)
    new_master = master_vals - LEARN_RATE * (new_mom / BIAS_ONE) / (jnp.sqrt(new_var / BIAS_TWO) + ADAM_EPS)
    return new_master, new_mom, new_var


def unpermute(shard):
    rows = shard.shape[1]
    return shard.reshape(NT, rows, OWN, PIECE).transpose(1, 2, 0, 3).reshape(rows, FF)


def solution(mesh):
    total_devices = mesh.shape['replica'] * mesh.shape['data']
    batch_spec = P(('replica', 'data'), None)
    whole_spec = P()
    shard_spec = P(None, 'data', None)

    def device_step(inp_rows, out_grad, w_up, w_down, master_up, master_down, mom_up, mom_down, var_up, var_down, clip_norm):
        w_upp = permute_columns(w_up)
        w_down5 = w_down.reshape(2, OWN, NT, PIECE, D)
        pre_one, mid_rows = forward(inp_rows, w_upp, w_down5)
        shard_down2, shard_up2, sqd, squ, dmid_rows, dmid_t = upper(
            mid_rows, mid_rows.T, out_grad, out_grad.T, w_upp, w_down5)
        shard_down1, shard_up1, _, _, square_sum = lower(
            sqd, squ, dmid_rows, dmid_t, inp_rows.T, pre_one, w_down5)
        grad_up = jnp.stack([unpermute(shard_up1), unpermute(shard_up2)]) / total_devices
        grad_down = jnp.stack([shard_down1.reshape(FF // OWN, D), shard_down2.reshape(FF // OWN, D)]) / total_devices
        grad_norm = jnp.sqrt(square_sum[0, 0]) / total_devices
        clip_scale = jnp.minimum(1.0, clip_norm / (grad_norm + NORM_EPS))
        master_up_new, mom_up_new, var_up_new = adam_update(grad_up, master_up, mom_up, var_up, clip_scale)
        master_down_new, mom_down_new, var_down_new = adam_update(grad_down, master_down, mom_down, var_down, clip_scale)
        w_up_new = lax.all_gather(master_up_new.astype(jnp.bfloat16), 'data', axis=1, tiled=True)
        w_down_new = lax.all_gather(master_down_new.astype(jnp.bfloat16), 'data', axis=1, tiled=True)
        return (w_up_new, w_down_new, master_up_new, master_down_new, mom_up_new, mom_down_new, var_up_new, var_down_new, grad_norm)

    return jax.shard_map(device_step, mesh=mesh, in_specs=(batch_spec, batch_spec, whole_spec, whole_spec, shard_spec, shard_spec, shard_spec, shard_spec, shard_spec, shard_spec, whole_spec), out_specs=(whole_spec, whole_spec, shard_spec, shard_spec, shard_spec, shard_spec, shard_spec, shard_spec, whole_spec), check_vma=False)
```

```python
import functools

import jax
import jax.numpy as jnp
from jax import lax
from jax.experimental import pallas as pl
from jax.experimental.pallas import tpu as pltpu
from jax.sharding import PartitionSpec as P

BETA1 = 0.9
BETA2 = 0.95
ADAM_EPS = 1e-8
LEARN_RATE = 5e-3
NORM_EPS = 1e-6
STEP = 10
BIAS_ONE = 1.0 - BETA1 ** STEP
BIAS_TWO = 1.0 - BETA2 ** STEP

F32 = jnp.float32
BF16 = jnp.bfloat16
ROWS = 4096
D = 896
FF = 4864
TILE = 256
NT = FF // TILE
OWN = 8
PIECE = TILE // OWN
RM = 512
NB = ROWS // RM
VMEM_LIMIT = 67_043_328


def gelu_value(pre_act):
    return pre_act * (0.5 + 0.5 * lax.erf(pre_act * 0.7071067811865476))


def gelu_both(pre_act):
    cdf = 0.5 + 0.5 * lax.erf(pre_act * 0.7071067811865476)
    return pre_act * cdf, cdf + pre_act * jnp.exp(-0.5 * pre_act * pre_act) * 0.3989422804014327


def mm(left, right):
    return jnp.dot(left, right, preferred_element_type=F32)


def mm_nt(left, right):
    return lax.dot_general(left, right, (((1,), (1,)), ((), ())), preferred_element_type=F32)


MESH = pl.DeviceIdType.MESH
LAG = 4
GRID = NT + LAG


def coordinates():
    d = lax.axis_index('data')
    z = lax.axis_index('replica')
    c = lax.rem(d, 2)
    x = lax.rem(lax.div(d, 2), 2)
    y = lax.div(d, 4)
    peers = {
        'c': {'data': d + 1 - 2 * c},
        'x': {'data': d + 2 - 4 * x},
        'y': {'data': d + 4 - 8 * y},
        'z': {'replica': 1 - z},
    }
    return d, c, x, y, z, peers


def neighbour_barrier(peers):
    barrier = pltpu.get_barrier_semaphore()
    for peer in peers:
        pl.semaphore_signal(barrier, inc=1, device_id=peer, device_id_type=MESH)
    pl.semaphore_wait(barrier, len(peers))


def grad_scratch(rows, cols):
    return [pltpu.VMEM((2, 2, 2, rows, cols), F32),
            pltpu.VMEM((2, 2, 2, rows, cols), F32),
            pltpu.VMEM((2, 2, rows, cols), F32),
            pltpu.VMEM((2, 2, rows, cols), F32),
            pltpu.VMEM((2, rows, cols), F32),
            pltpu.VMEM((2, rows, cols), F32),
            pltpu.VMEM((rows, cols), F32),
            pltpu.VMEM((2, rows, cols), F32),
            pltpu.SemaphoreType.DMA((4, 2)),
            pltpu.SemaphoreType.DMA((4, 2))]


class Reducer:
    def __init__(self, scratch, x_first, t):
        (self.tile, self.in_core, self.chip, self.in_one, self.two, self.in_two, self.four, self.in_rep,
         self.send, self.recv) = scratch
        self.x_first = x_first
        self.t = t
        _, self.c, self.x, self.y, _, self.peers = coordinates()

    def copy(self, stage, tile_index):
        slot = lax.rem(tile_index + 2, 2)
        first, second = ('x', 'y') if self.x_first else ('y', 'x')
        if stage == 0:
            src, dst, peer = self.tile.at[:, :, 1 - self.c], self.in_core.at[slot], 'c'
        elif stage == 1:
            src = self.chip.at[:, 1 - self.x] if self.x_first else self.chip.at[1 - self.y]
            dst, peer = self.in_one.at[slot], first
        elif stage == 2:
            src = self.two.at[1 - self.y] if self.x_first else self.two.at[1 - self.x]
            dst, peer = self.in_two.at[slot], second
        else:
            src, dst, peer = self.four, self.in_rep.at[slot], 'z'
        return pltpu.make_async_remote_copy(
            src_ref=src, dst_ref=dst, send_sem=self.send.at[stage, slot], recv_sem=self.recv.at[stage, slot],
            device_id=self.peers[peer], device_id_type=MESH)

    def start(self):
        self.copy(0, self.t).start()

    def progress(self, out_ref, sq_ref):
        t = self.t

        @pl.when(t >= 4)
        def _():
            self.copy(3, t - 4).wait()
            total = self.four[...] + self.in_rep[lax.rem(t, 2)]
            out_ref[0] = total
            sq_ref[...] += jnp.sum(total * total, axis=0, keepdims=True)

        @pl.when((t >= 3) & (t < NT + 3))
        def _():
            self.copy(2, t - 3).wait()
            mine = self.two[self.y] if self.x_first else self.two[self.x]
            self.four[...] = mine + self.in_two[lax.rem(t + 1, 2)]
            self.copy(3, t - 3).start()

        @pl.when((t >= 2) & (t < NT + 2))
        def _():
            self.copy(1, t - 2).wait()
            mine = self.chip[:, self.x] if self.x_first else self.chip[self.y]
            self.two[...] = mine + self.in_one[lax.rem(t, 2)]
            self.copy(2, t - 2).start()

        @pl.when((t >= 1) & (t < NT + 1))
        def _():
            self.copy(0, t - 1).wait()
            self.chip[...] = self.tile[:, :, self.c] + self.in_core[lax.rem(t + 1, 2)]
            self.copy(1, t - 1).start()


def permute_kernel(w_ref, out_ref):
    for t in range(NT):
        out_ref[:, t * TILE:(t + 1) * TILE] = jnp.concatenate(
            [w_ref[:, d * (FF // OWN) + t * PIECE:d * (FF // OWN) + (t + 1) * PIECE] for d in range(OWN)], axis=1)


def permute_columns(w_up):
    rows = 128
    flat = w_up.reshape(2 * D, FF)
    out = pl.pallas_call(
        permute_kernel,
        grid=(2 * D // rows,),
        in_specs=[pl.BlockSpec((rows, FF), lambda i: (i, 0))],
        out_specs=pl.BlockSpec((rows, FF), lambda i: (i, 0)),
        out_shape=jax.ShapeDtypeStruct((2 * D, FF), w_up.dtype),
        name="permute_columns",
    )(flat)
    return out.reshape(2, D, FF)


def forward_kernel(x_ref, dy_ref, wu_ref, wd_ref, z_ref, h_ref, ht_ref, xt_ref, dyt_ref, acc):
    t = pl.program_id(0)
    block = jnp.minimum(t, ROWS // TILE - 1)

    @pl.when(t == 0)
    def _():
        acc[...] = jnp.zeros_like(acc)

    wd = wd_ref[0, :, 0].reshape(TILE, D)
    for r in range(NB + 1):
        if r < NB:
            rows = pl.ds(r * RM, RM)
            z_ref[0, rows, :] = mm(x_ref[rows, :], wu_ref[0]).astype(BF16)
        if r > 0:
            rows = pl.ds((r - 1) * RM, RM)
            u = gelu_value(z_ref[0, rows, :].astype(F32)).astype(BF16)
            acc[rows, :] += mm(u, wd)
        if r == 2:
            xt_ref[...] = x_ref[pl.ds(pl.multiple_of(block * TILE, TILE), TILE), :].T
        if r == 5:
            dyt_ref[...] = dy_ref[...].T

    @pl.when(t == NT - 1)
    def _():
        h_ref[...] = acc[...].astype(BF16)
        ht_ref[...] = h_ref[...].T


def forward(x, dy, w_upp, w_down5):
    last = ROWS // TILE - 1
    once = pl.Buffered(1)
    return pl.pallas_call(
        forward_kernel,
        grid=(NT,),
        in_specs=[
            pl.BlockSpec((ROWS, D), lambda t: (0, 0), pipeline_mode=once),
            pl.BlockSpec((TILE, D), lambda t: (jnp.minimum(t, last), 0)),
            pl.BlockSpec((1, D, TILE), lambda t: (0, 0, t)),
            pl.BlockSpec((1, OWN, 1, PIECE, D), lambda t: (0, 0, t, 0, 0)),
        ],
        out_specs=[
            pl.BlockSpec((1, ROWS, TILE), lambda t: (t, 0, 0)),
            pl.BlockSpec((ROWS, D), lambda t: (0, 0), pipeline_mode=once),
            pl.BlockSpec((D, ROWS), lambda t: (0, 0), pipeline_mode=once),
            pl.BlockSpec((D, TILE), lambda t: (0, jnp.minimum(t, last))),
            pl.BlockSpec((D, TILE), lambda t: (0, jnp.minimum(t, last))),
        ],
        out_shape=[jax.ShapeDtypeStruct((NT, ROWS, TILE), BF16), jax.ShapeDtypeStruct((ROWS, D), BF16),
                   jax.ShapeDtypeStruct((D, ROWS), BF16), jax.ShapeDtypeStruct((D, ROWS), BF16),
                   jax.ShapeDtypeStruct((D, ROWS), BF16)],
        scratch_shapes=[pltpu.VMEM((ROWS, D), F32)],
        compiler_params=pltpu.CompilerParams(vmem_limit_bytes=VMEM_LIMIT),
        name="forward",
    )(x, dy, w_upp, w_down5)


def upper_kernel(h_hbm, ht_hbm, dy_hbm, dyt_hbm, wu_ref, wd_ref, gd_ref, gu_ref, sqd_ref, squ_ref, dh_hbm, dht_hbm,
                 h, ht, dy, dyt, acc, u_s, d_s, sems, *grads):
    t = pl.program_id(0)
    loads = [pltpu.make_async_copy(s, v, sems.at[i]) for i, (s, v) in
             enumerate([(h_hbm, h), (dy_hbm, dy), (dyt_hbm, dyt), (ht_hbm, ht)])]
    stores = [pltpu.make_async_copy(h, dh_hbm, sems.at[0]), pltpu.make_async_copy(ht, dht_hbm, sems.at[1])]
    down = Reducer(grads[:10], True, t)
    up = Reducer(grads[10:], False, t)

    @pl.when(t == 0)
    def _():
        for copy in loads:
            copy.start()
        neighbour_barrier([down.peers[k] for k in 'cxyz'])
        acc[...] = jnp.zeros_like(acc)
        sqd_ref[...] = jnp.zeros_like(sqd_ref)
        squ_ref[...] = jnp.zeros_like(squ_ref)
        loads[0].wait()
        loads[1].wait()

    def rows_of(first, last):
        wu = wu_ref[0]
        wd = wd_ref[0, :, 0].reshape(TILE, D)
        for r in range(first, last):
            if r < NB:
                rows = pl.ds(r * RM, RM)
                u_s[rows, :] = mm(h[rows, :], wu).astype(BF16)
                d_s[rows, :] = mm_nt(dy[rows, :], wd).astype(BF16)
            if r > 0:
                rows = pl.ds((r - 1) * RM, RM)
                u, slope = gelu_both(u_s[rows, :].astype(F32))
                dz = (d_s[rows, :].astype(F32) * slope).astype(BF16)
                u_s[rows, :] = u.astype(BF16)
                d_s[rows, :] = dz
                acc[rows, :] += mm_nt(dz, wu)

    @pl.when(t < NT)
    def _():
        rows_of(0, NB // 2)

    down.progress(gd_ref, sqd_ref)

    @pl.when(t < NT)
    def _():
        rows_of(NB // 2, NB + 1)

    up.progress(gu_ref, squ_ref)

    @pl.when(t == 0)
    def _():
        loads[2].wait()
        loads[3].wait()

    @pl.when(t < NT)
    def _():
        down.tile[...] = mm(dyt[...], u_s[...]).T.reshape(2, 2, 2, PIECE, D)
        up.tile[...] = mm(ht[...], d_s[...]).reshape(2, 2, 2, D // OWN, TILE)
        down.start()
        up.start()

    @pl.when(t == NT - 1)
    def _():
        h[...] = acc[...].astype(BF16)
        stores[0].start()

    @pl.when(t == NT)
    def _():
        ht[...] = h[...].T
        stores[1].start()

    @pl.when(t == GRID - 1)
    def _():
        stores[0].wait()
        stores[1].wait()


def final_tile(t):
    return jnp.clip(t - LAG, 0, NT - 1)


def this_tile(t):
    return jnp.minimum(t, NT - 1)


GRAD_SPECS = [
    pl.BlockSpec((1, PIECE, D), lambda t: (final_tile(t), 0, 0)),
    pl.BlockSpec((1, D // OWN, TILE), lambda t: (final_tile(t), 0, 0)),
    pl.BlockSpec((1, D), lambda t: (0, 0)),
    pl.BlockSpec((1, TILE), lambda t: (0, 0)),
]
GRAD_SHAPES = [
    jax.ShapeDtypeStruct((NT, PIECE, D), F32),
    jax.ShapeDtypeStruct((NT, D // OWN, TILE), F32),
    jax.ShapeDtypeStruct((1, D), F32),
    jax.ShapeDtypeStruct((1, TILE), F32),
]


def upper(h, ht, dy, dyt, w_upp, w_down5):
    anyspec = pl.BlockSpec(memory_space=pl.ANY)
    return pl.pallas_call(
        upper_kernel,
        grid=(GRID,),
        in_specs=[anyspec] * 4 + [
            pl.BlockSpec((1, D, TILE), lambda t: (1, 0, this_tile(t))),
            pl.BlockSpec((1, OWN, 1, PIECE, D), lambda t: (1, 0, this_tile(t), 0, 0)),
        ],
        out_specs=GRAD_SPECS + [anyspec, anyspec],
        out_shape=GRAD_SHAPES + [jax.ShapeDtypeStruct((ROWS, D), BF16), jax.ShapeDtypeStruct((D, ROWS), BF16)],
        scratch_shapes=[pltpu.VMEM((ROWS, D), BF16), pltpu.VMEM((D, ROWS), BF16),
                        pltpu.VMEM((ROWS, D), BF16), pltpu.VMEM((D, ROWS), BF16),
                        pltpu.VMEM((ROWS, D), F32), pltpu.VMEM((ROWS, TILE), BF16), pltpu.VMEM((ROWS, TILE), BF16),
                        pltpu.SemaphoreType.DMA((4,))] + grad_scratch(PIECE, D) + grad_scratch(D // OWN, TILE),
        compiler_params=pltpu.CompilerParams(vmem_limit_bytes=VMEM_LIMIT, collective_id=0, has_side_effects=True),
        name="upper",
    )(h, ht, dy, dyt, w_upp, w_down5)


def lower_kernel(sqd_in, squ_in, dh_hbm, dht_hbm, xt_hbm, z_ref, wd_ref, gd_ref, gu_ref, sqd_ref, squ_ref, norm_ref,
                 dh, dht, xt, u_s, d_s, sems, sq_mine, sq_all, sq_send, sq_recv, *grads):
    t = pl.program_id(0)
    loads = [pltpu.make_async_copy(s, v, sems.at[i]) for i, (s, v) in
             enumerate([(dh_hbm, dh), (dht_hbm, dht), (xt_hbm, xt)])]
    down = Reducer(grads[:10], True, t)
    up = Reducer(grads[10:], False, t)
    me = lax.axis_index('data')
    others = [{'data': lax.rem(me + k, OWN)} for k in range(1, OWN)]

    @pl.when(t == 0)
    def _():
        for copy in loads:
            copy.start()
        neighbour_barrier(others + [down.peers['z']])
        sqd_ref[...] = sqd_in[...]
        squ_ref[...] = squ_in[...]
        loads[0].wait()

    def rows_of(first, last):
        wd = wd_ref[0, :, 0].reshape(TILE, D)
        for r in range(first, last):
            if r < NB:
                rows = pl.ds(r * RM, RM)
                d_s[rows, :] = mm_nt(dh[rows, :], wd).astype(BF16)
            if r > 0:
                rows = pl.ds((r - 1) * RM, RM)
                u, slope = gelu_both(z_ref[0, rows, :].astype(F32))
                u_s[rows, :] = u.astype(BF16)
                d_s[rows, :] = (d_s[rows, :].astype(F32) * slope).astype(BF16)

    @pl.when(t < NT)
    def _():
        rows_of(0, NB // 2)

    down.progress(gd_ref, sqd_ref)

    @pl.when(t < NT)
    def _():
        rows_of(NB // 2, NB + 1)

    up.progress(gu_ref, squ_ref)

    @pl.when(t == 0)
    def _():
        loads[1].wait()
        loads[2].wait()

    @pl.when(t < NT)
    def _():
        down.tile[...] = mm(dht[...], u_s[...]).T.reshape(2, 2, 2, PIECE, D)
        up.tile[...] = mm(xt[...], d_s[...]).reshape(2, 2, 2, D // OWN, TILE)
        down.start()
        up.start()

    @pl.when(t == GRID - 1)
    def _():
        part = jnp.sum(sqd_ref[...], axis=1, keepdims=True) + jnp.sum(squ_ref[...], axis=1, keepdims=True)
        sq_mine[...] = jnp.broadcast_to(part, sq_mine.shape)
        sq_all[me] = sq_mine[...]
        copies = [pltpu.make_async_remote_copy(
            src_ref=sq_mine, dst_ref=sq_all.at[me], send_sem=sq_send.at[k], recv_sem=sq_recv.at[k],
            device_id=others[k], device_id_type=MESH) for k in range(OWN - 1)]
        for copy in copies:
            copy.start()
        for copy in copies:
            copy.wait()
        total = sq_all[0]
        for k in range(1, OWN):
            total = total + sq_all[k]
        norm_ref[...] = total


def lower(sqd, squ, dh, dht, xt, z, w_down5):
    anyspec = pl.BlockSpec(memory_space=pl.ANY)
    return pl.pallas_call(
        lower_kernel,
        grid=(GRID,),
        in_specs=GRAD_SPECS[2:] + [anyspec] * 3 + [
            pl.BlockSpec((1, ROWS, TILE), lambda t: (this_tile(t), 0, 0)),
            pl.BlockSpec((1, OWN, 1, PIECE, D), lambda t: (0, 0, this_tile(t), 0, 0)),
        ],
        out_specs=GRAD_SPECS + [pl.BlockSpec((8, 128), lambda t: (0, 0))],
        out_shape=GRAD_SHAPES + [jax.ShapeDtypeStruct((8, 128), F32)],
        scratch_shapes=[pltpu.VMEM((ROWS, D), BF16), pltpu.VMEM((D, ROWS), BF16), pltpu.VMEM((D, ROWS), BF16),
                        pltpu.VMEM((ROWS, TILE), BF16), pltpu.VMEM((ROWS, TILE), BF16),
                        pltpu.SemaphoreType.DMA((3,)),
                        pltpu.VMEM((8, 128), F32), pltpu.VMEM((OWN, 8, 128), F32),
                        pltpu.SemaphoreType.DMA((OWN - 1,)), pltpu.SemaphoreType.DMA((OWN - 1,))]
        + grad_scratch(PIECE, D) + grad_scratch(D // OWN, TILE),
        compiler_params=pltpu.CompilerParams(vmem_limit_bytes=VMEM_LIMIT, collective_id=1, has_side_effects=True),
        name="lower",
    )(sqd, squ, dh, dht, xt, z, w_down5)


def adam_update(grad_vals, master_vals, mom_vals, var_vals, clip_scale):
    new_mom = BETA1 * mom_vals + (1.0 - BETA1) * clip_scale * grad_vals
    new_var = BETA2 * var_vals + (1.0 - BETA2) * (clip_scale * clip_scale) * (grad_vals * grad_vals)
    new_master = master_vals - LEARN_RATE * (new_mom / BIAS_ONE) / (jnp.sqrt(new_var / BIAS_TWO) + ADAM_EPS)
    return new_master, new_mom, new_var


def norm_and_clip(sq_ref, clip_ref):
    norm = jnp.sqrt(sq_ref[...]) / DEVICES
    return norm, jnp.minimum(1.0, clip_ref[0, 0] / (norm + NORM_EPS))[0:1, 0:1]


UP_ROWS = D // OWN
DOWN_ROWS = FF // OWN
DEVICES = 16


def adam_up_kernel(sq_ref, clip_ref, one_ref, two_ref, master_ref, mom_ref, var_ref,
                   new_w_ref, new_master_ref, new_mom_ref, new_var_ref):
    _, scale = norm_and_clip(sq_ref, clip_ref)

    def update(g_ref):
        for n in range(FF // 128):
            pieces = [divmod(4 * n + q, NT) for q in range(4)]
            grad = jnp.concatenate([g_ref[t, :, d * PIECE:(d + 1) * PIECE] for d, t in pieces], axis=1) / DEVICES
            cols = pl.ds(n * 128, 128)
            master, mom, var = adam_update(grad, master_ref[0, :, cols], mom_ref[0, :, cols], var_ref[0, :, cols], scale)
            new_master_ref[0, :, cols] = master
            new_mom_ref[0, :, cols] = mom
            new_var_ref[0, :, cols] = var
            new_w_ref[0, :, cols] = master.astype(BF16)

    pl.when(pl.program_id(0) == 0)(lambda: update(one_ref))
    pl.when(pl.program_id(0) == 1)(lambda: update(two_ref))


def adam_down_kernel(sq_ref, clip_ref, one_ref, two_ref, master_ref, mom_ref, var_ref,
                     new_w_ref, new_master_ref, new_mom_ref, new_var_ref, norm_ref):
    norm, scale = norm_and_clip(sq_ref, clip_ref)
    norm_ref[...] = norm

    def update(g_ref):
        def body(i, carry):
            rows = pl.ds(pl.multiple_of(i * 16, 16), 16)
            master, mom, var = adam_update(g_ref[rows, :] / DEVICES, master_ref[0, rows, :], mom_ref[0, rows, :],
                                           var_ref[0, rows, :], scale)
            new_master_ref[0, rows, :] = master
            new_mom_ref[0, rows, :] = mom
            new_var_ref[0, rows, :] = var
            new_w_ref[0, rows, :] = master.astype(BF16)
            return carry

        lax.fori_loop(0, g_ref.shape[0] // 16, body, 0)

    pl.when(pl.program_id(0) == 0)(lambda: update(one_ref))
    pl.when(pl.program_id(0) == 1)(lambda: update(two_ref))


def adam_call(kernel, name, square_sum, clip, g_one, g_two, master, mom, var, block, g_block, with_norm):
    layers, rows, cols = master.shape
    steps = rows // block
    dims = len(g_block)

    def state_index(layer, i):
        return (layer, i, 0)

    def g_index(which):
        def index(layer, i):
            fixed = jnp.where(layer == which, i, steps - 1 if which == 0 else 0)
            return (0, fixed, 0) if dims == 3 else (fixed, 0)
        return index

    state = pl.BlockSpec((1, block, cols), state_index)
    small = pl.BlockSpec((8, 128), lambda layer, i: (0, 0))
    out_specs = [state] * 4 + ([small] if with_norm else [])
    out_shape = [jax.ShapeDtypeStruct(master.shape, BF16)] + [jax.ShapeDtypeStruct(master.shape, F32)] * 3
    if with_norm:
        out_shape = out_shape + [jax.ShapeDtypeStruct((8, 128), F32)]
    return pl.pallas_call(
        kernel,
        grid=(layers, steps),
        in_specs=[small, pl.BlockSpec(memory_space=pltpu.SMEM),
                  pl.BlockSpec(g_block, g_index(0)), pl.BlockSpec(g_block, g_index(1)), state, state, state],
        out_specs=out_specs,
        out_shape=out_shape,
        compiler_params=pltpu.CompilerParams(vmem_limit_bytes=VMEM_LIMIT),
        name=name,
    )(square_sum, clip, g_one, g_two, master, mom, var)


UP_CHUNKS = [(True, 0, 16), (True, 16, 32), (True, 48, 32), (True, 80, 32)]
DOWN_CHUNKS = [(False, 0, 144), (False, 144, 144), (False, 288, 160), (False, 448, 160)]
CHUNKS = UP_CHUNKS + DOWN_CHUNKS
NC = len(CHUNKS)
GROUPS = 14


def gather_kernel(up_hbm, down_hbm, out_up, out_down, up_v, down_v, send, recv, local):
    d, c, x, y, z, peers = coordinates()
    d_x = d + 2 - 4 * x
    d_y = d + 4 - 8 * y
    d_xy = d_x + 4 - 8 * y
    other_core = 1 - 2 * c

    loads = [pltpu.make_async_copy(up_hbm, up_v, local.at[0]), pltpu.make_async_copy(down_hbm, down_v, local.at[1])]
    for copy in loads:
        copy.start()
    neighbour_barrier([peers[k] for k in 'cxyz'])
    for copy in loads:
        copy.wait()

    def region(chunk, layer, owner):
        is_up, first, count = CHUNKS[chunk]
        out, rows = (out_up, UP_ROWS) if is_up else (out_down, DOWN_ROWS)
        return out.at[layer, pl.ds(pl.multiple_of(owner * rows + first, 16), count)]

    def mine(chunk, layer):
        is_up, first, count = CHUNKS[chunk]
        return (up_v if is_up else down_v).at[layer, pl.ds(first, count)]

    started = []

    def send_chunk(group, chunk, src, layer, owner, peer):
        copy = pltpu.make_async_remote_copy(
            src_ref=src, dst_ref=region(chunk, layer, owner), send_sem=send.at[group, chunk],
            recv_sem=recv.at[group, chunk], device_id=peers[peer], device_id_type=MESH)
        copy.start()
        started.append(copy)

    def arrived(group, chunk, layer, owner):
        pltpu.make_async_remote_copy(
            src_ref=region(chunk, layer, owner), dst_ref=region(chunk, layer, owner), send_sem=send.at[group, chunk],
            recv_sem=recv.at[group, chunk], device_id=peers['c'], device_id_type=MESH).wait_recv()

    for k in range(NC):
        send_chunk(0, k, mine(k, z), z, d, 'x')
        send_chunk(1, k, mine(k, 1 - z), 1 - z, d, 'y')
    for k in range(NC):
        send_chunk(6, k, mine(k, 0), 0, d, 'c')
        send_chunk(7, k, mine(k, 1), 1, d, 'c')
    stores = []
    for layer in range(2):
        stores.append(pltpu.make_async_copy(up_v.at[layer], out_up.at[layer, pl.ds(pl.multiple_of(d * UP_ROWS, 16), UP_ROWS)], local.at[2 + layer]))
        stores.append(pltpu.make_async_copy(down_v.at[layer], out_down.at[layer, pl.ds(pl.multiple_of(d * DOWN_ROWS, 16), DOWN_ROWS)], local.at[4 + layer]))
    for copy in stores:
        copy.start()

    def second(k):
        for group, core_group, layer, owner in ((4, 10, 1 - z, d_x), (5, 11, z, d_y), (2, 12, z, d_xy), (3, 13, 1 - z, d_xy)):
            arrived(group, k, layer, owner)
            send_chunk(core_group, k, region(k, layer, owner), layer, owner, 'c')

    for k in range(NC):
        arrived(0, k, z, d_x)
        src = region(k, z, d_x)
        send_chunk(4, k, src, z, d_x, 'z')
        send_chunk(2, k, src, z, d_x, 'y')
        send_chunk(8, k, src, z, d_x, 'c')
        arrived(1, k, 1 - z, d_y)
        src = region(k, 1 - z, d_y)
        send_chunk(5, k, src, 1 - z, d_y, 'z')
        send_chunk(3, k, src, 1 - z, d_y, 'x')
        send_chunk(9, k, src, 1 - z, d_y, 'c')
    for k in range(NC):
        second(k)
    for k in range(NC):
        for group, layer, owner in ((6, 0, d), (7, 1, d), (8, z, d_x), (9, 1 - z, d_y), (10, 1 - z, d_x),
                                    (11, z, d_y), (12, z, d_xy), (13, 1 - z, d_xy)):
            arrived(group, k, layer, owner + other_core)
    for copy in started:
        copy.wait_send()
    for copy in stores:
        copy.wait()


def gather(up_shard, down_shard):
    anyspec = pl.BlockSpec(memory_space=pl.ANY)
    return pl.pallas_call(
        gather_kernel,
        in_specs=[anyspec, anyspec],
        out_specs=[anyspec, anyspec],
        out_shape=[jax.ShapeDtypeStruct((2, D, FF), BF16), jax.ShapeDtypeStruct((2, FF, D), BF16)],
        scratch_shapes=[pltpu.VMEM((2, UP_ROWS, FF), BF16), pltpu.VMEM((2, DOWN_ROWS, D), BF16),
                        pltpu.SemaphoreType.DMA((GROUPS, NC)), pltpu.SemaphoreType.DMA((GROUPS, NC)),
                        pltpu.SemaphoreType.DMA((6,))],
        compiler_params=pltpu.CompilerParams(vmem_limit_bytes=VMEM_LIMIT, collective_id=2, has_side_effects=True),
        name="gather",
    )(up_shard, down_shard)


def solution(mesh):
    batch_spec = P(('replica', 'data'), None)
    whole_spec = P()
    shard_spec = P(None, 'data', None)

    def device_step(inp_rows, out_grad, w_up, w_down, master_up, master_down, mom_up, mom_down, var_up, var_down, clip_norm):
        w_upp = permute_columns(w_up)
        w_down5 = w_down.reshape(2, OWN, NT, PIECE, D)
        pre_one, mid_rows, mid_t, inp_t, grad_t = forward(inp_rows, out_grad, w_upp, w_down5)
        shard_down2, shard_up2, sqd, squ, dmid_rows, dmid_t = upper(mid_rows, mid_t, out_grad, grad_t, w_upp, w_down5)
        shard_down1, shard_up1, _, _, square_sum = lower(sqd, squ, dmid_rows, dmid_t, inp_t, pre_one, w_down5)
        clip = clip_norm.reshape(1, 1)
        w_up_shard, master_up_new, mom_up_new, var_up_new = adam_call(
            adam_up_kernel, "adam_up", square_sum, clip, shard_up1, shard_up2, master_up, mom_up, var_up,
            16, (NT, 16, TILE), False)
        w_down_shard, master_down_new, mom_down_new, var_down_new, norm = adam_call(
            adam_down_kernel, "adam_down", square_sum, clip, shard_down1.reshape(DOWN_ROWS, D),
            shard_down2.reshape(DOWN_ROWS, D), master_down, mom_down, var_down, 304, (304, D), True)
        w_up_new, w_down_new = gather(w_up_shard, w_down_shard)
        return (w_up_new, w_down_new, master_up_new, master_down_new, mom_up_new, mom_down_new, var_up_new, var_down_new, norm[0, 0])

    return jax.shard_map(device_step, mesh=mesh, in_specs=(batch_spec, batch_spec, whole_spec, whole_spec, shard_spec, shard_spec, shard_spec, shard_spec, shard_spec, shard_spec, whole_spec), out_specs=(whole_spec, whole_spec, shard_spec, shard_spec, shard_spec, shard_spec, shard_spec, shard_spec, whole_spec), check_vma=False)
```

```python
import functools

import jax
import jax.numpy as jnp
from jax import lax
from jax.experimental import pallas as pl
from jax.experimental.pallas import tpu as pltpu
from jax.sharding import PartitionSpec as P

BETA1 = 0.9
BETA2 = 0.95
ADAM_EPS = 1e-8
LEARN_RATE = 5e-3
NORM_EPS = 1e-6
STEP = 10
BIAS_ONE = 1.0 - BETA1 ** STEP
BIAS_TWO = 1.0 - BETA2 ** STEP

F32 = jnp.float32
BF16 = jnp.bfloat16
ROWS = 4096
D = 896
FF = 4864
TILE = 256
NT = FF // TILE
OWN = 8
PIECE = TILE // OWN
UP_ROWS = D // OWN
DOWN_ROWS = FF // OWN
DEVICES = 16
RM = 256
NB = ROWS // RM
VMEM_LIMIT = 67_043_328


def gelu_value(pre_act):
    return pre_act * (0.5 + 0.5 * lax.erf(pre_act * 0.7071067811865476))


def gelu_both(pre_act):
    scaled = pre_act * 0.7071067811865476
    cdf = 0.5 + 0.5 * lax.erf(scaled)
    return pre_act * cdf, cdf + pre_act * jnp.exp2(scaled * scaled * -1.4426950408889634) * 0.3989422804014327


def mm(left, right):
    return jnp.dot(left, right, preferred_element_type=F32)


def mm_nt(left, right):
    return lax.dot_general(left, right, (((1,), (1,)), ((), ())), preferred_element_type=F32)


MESH = pl.DeviceIdType.MESH
LAG = 4
TILES = 2 * NT
GRID = TILES + LAG
EARLY = 6


def coordinates():
    d = lax.axis_index('data')
    z = lax.axis_index('replica')
    c = lax.rem(d, 2)
    x = lax.rem(lax.div(d, 2), 2)
    y = lax.div(d, 4)
    peers = {
        'c': {'data': d + 1 - 2 * c},
        'x': {'data': d + 2 - 4 * x},
        'y': {'data': d + 4 - 8 * y},
        'z': {'replica': 1 - z},
    }
    return d, c, x, y, z, peers


def neighbour_barrier(peers):
    barrier = pltpu.get_barrier_semaphore()
    for peer in peers:
        pl.semaphore_signal(barrier, inc=1, device_id=peer, device_id_type=MESH)
    pl.semaphore_wait(barrier, len(peers))


def grad_scratch(rows, cols):
    return [pltpu.VMEM((2, 2, 2, rows, cols), F32),
            pltpu.VMEM((2, 2, 2, rows, cols), F32),
            pltpu.VMEM((2, 2, rows, cols), F32),
            pltpu.VMEM((2, 2, rows, cols), F32),
            pltpu.VMEM((2, rows, cols), F32),
            pltpu.VMEM((2, rows, cols), F32),
            pltpu.VMEM((rows, cols), F32),
            pltpu.VMEM((2, rows, cols), F32),
            pltpu.SemaphoreType.DMA((4, 2)),
            pltpu.SemaphoreType.DMA((4, 2))]


class Reducer:
    def __init__(self, scratch, x_first, t):
        (self.tile, self.in_core, self.chip, self.in_one, self.two, self.in_two, self.four, self.in_rep,
         self.send, self.recv) = scratch
        self.x_first = x_first
        self.t = t
        _, self.c, self.x, self.y, _, self.peers = coordinates()

    def copy(self, stage, tile_index):
        slot = lax.rem(tile_index + 2, 2)
        first, second = ('x', 'y') if self.x_first else ('y', 'x')
        if stage == 0:
            src, dst, peer = self.tile.at[:, :, 1 - self.c], self.in_core.at[slot], 'c'
        elif stage == 1:
            src = self.chip.at[:, 1 - self.x] if self.x_first else self.chip.at[1 - self.y]
            dst, peer = self.in_one.at[slot], first
        elif stage == 2:
            src = self.two.at[1 - self.y] if self.x_first else self.two.at[1 - self.x]
            dst, peer = self.in_two.at[slot], second
        else:
            src, dst, peer = self.four, self.in_rep.at[slot], 'z'
        return pltpu.make_async_remote_copy(
            src_ref=src, dst_ref=dst, send_sem=self.send.at[stage, slot], recv_sem=self.recv.at[stage, slot],
            device_id=self.peers[peer], device_id_type=MESH)

    def start(self):
        self.copy(0, self.t).start()

    def progress(self, out_ref, sq_ref):
        t = self.t

        @pl.when(t >= 4)
        def _():
            self.copy(3, t - 4).wait()
            total = self.four[...] + self.in_rep[lax.rem(t, 2)]
            out_ref[0] = total
            sq_ref[...] += jnp.sum((total * total).reshape(-1, 8, total.shape[1]), axis=0)

        @pl.when((t >= 3) & (t < TILES + 3))
        def _():
            self.copy(2, t - 3).wait()
            mine = self.two[self.y] if self.x_first else self.two[self.x]
            self.four[...] = mine + self.in_two[lax.rem(t + 1, 2)]
            self.copy(3, t - 3).start()

        @pl.when((t >= 2) & (t < TILES + 2))
        def _():
            self.copy(1, t - 2).wait()
            mine = self.chip[:, self.x] if self.x_first else self.chip[self.y]
            self.two[...] = mine + self.in_one[lax.rem(t, 2)]
            self.copy(2, t - 2).start()

        @pl.when((t >= 1) & (t < TILES + 1))
        def _():
            self.copy(0, t - 1).wait()
            self.chip[...] = self.tile[:, :, self.c] + self.in_core[lax.rem(t + 1, 2)]
            self.copy(1, t - 1).start()


def permuted(w_ref, out_ref):
    for t in range(NT):
        out_ref[:, t * TILE:(t + 1) * TILE] = jnp.concatenate(
            [w_ref[0, :, d * DOWN_ROWS + t * PIECE:d * DOWN_ROWS + (t + 1) * PIECE] for d in range(OWN)], axis=1)


PERM_ROWS = 64


def permute_first(w_up):
    return pl.pallas_call(
        permuted,
        grid=(D // PERM_ROWS,),
        in_specs=[pl.BlockSpec((1, PERM_ROWS, FF), lambda i: (0, i, 0))],
        out_specs=pl.BlockSpec((PERM_ROWS, FF), lambda i: (i, 0)),
        out_shape=jax.ShapeDtypeStruct((D, FF), w_up.dtype),
        name="permute_first",
    )(w_up)


def forward_kernel(x_ref, dy_ref, wu_ref, wd_ref, next_ref, z_ref, h_ref, ht_ref, xt_ref, dyt_ref, next_out, acc):
    t = pl.program_id(0)
    block = jnp.minimum(t, ROWS // TILE - 1)

    @pl.when(t == 0)
    def _():
        acc[...] = jnp.zeros_like(acc)

    wd = wd_ref[0, :, 0].reshape(TILE, D)
    permuted(next_ref, next_out)
    for r in range(NB + 1):
        if r < NB:
            rows = pl.ds(r * RM, RM)
            z_ref[0, rows, :] = mm(x_ref[rows, :], wu_ref[...]).astype(BF16)
        if r > 0:
            rows = pl.ds((r - 1) * RM, RM)
            u = gelu_value(z_ref[0, rows, :].astype(F32)).astype(BF16)
            acc[rows, :] += mm(u, wd)
        if r == 2:
            xt_ref[...] = x_ref[pl.ds(pl.multiple_of(block * TILE, TILE), TILE), :].T
        if r == 5:
            dyt_ref[...] = dy_ref[...].T

    @pl.when(t == NT - 1)
    def _():
        h_ref[...] = acc[...].astype(BF16)
        ht_ref[...] = h_ref[...].T


def forward(x, dy, w_one, w_down5, w_up):
    last = ROWS // TILE - 1
    last_perm = D // PERM_ROWS - 1
    once = pl.Buffered(1)
    return pl.pallas_call(
        forward_kernel,
        grid=(NT,),
        in_specs=[
            pl.BlockSpec((ROWS, D), lambda t: (0, 0), pipeline_mode=once),
            pl.BlockSpec((TILE, D), lambda t: (jnp.minimum(t, last), 0)),
            pl.BlockSpec((D, TILE), lambda t: (0, t)),
            pl.BlockSpec((1, OWN, 1, PIECE, D), lambda t: (0, 0, t, 0, 0)),
            pl.BlockSpec((1, PERM_ROWS, FF), lambda t: (1, jnp.minimum(t, last_perm), 0)),
        ],
        out_specs=[
            pl.BlockSpec((1, ROWS, TILE), lambda t: (t, 0, 0)),
            pl.BlockSpec((ROWS, D), lambda t: (0, 0), pipeline_mode=once),
            pl.BlockSpec((D, ROWS), lambda t: (0, 0), pipeline_mode=once),
            pl.BlockSpec((D, TILE), lambda t: (0, jnp.minimum(t, last))),
            pl.BlockSpec((D, TILE), lambda t: (0, jnp.minimum(t, last))),
            pl.BlockSpec((PERM_ROWS, FF), lambda t: (jnp.minimum(t, last_perm), 0)),
        ],
        out_shape=[jax.ShapeDtypeStruct((NT, ROWS, TILE), BF16), jax.ShapeDtypeStruct((ROWS, D), BF16),
                   jax.ShapeDtypeStruct((D, ROWS), BF16), jax.ShapeDtypeStruct((D, ROWS), BF16),
                   jax.ShapeDtypeStruct((D, ROWS), BF16), jax.ShapeDtypeStruct((D, FF), BF16)],
        scratch_shapes=[pltpu.VMEM((ROWS, D), F32)],
        compiler_params=pltpu.CompilerParams(vmem_limit_bytes=VMEM_LIMIT),
        name="forward",
    )(x, dy, w_one, w_down5, w_up)


def backward_kernel(h_hbm, ht_hbm, dy_hbm, dyt_hbm, xt_hbm, wu_ref, wd_ref, z_ref, gd_ref, gu_ref, norm_ref,
                    h, ht, dy, dyt, acc, u_s, d_s, part_down, part_up, sq_down, sq_up, sems,
                    sq_mine, sq_all, sq_send, sq_recv, *grads):
    t = pl.program_id(0)
    loads = [pltpu.make_async_copy(s, v, sems.at[i]) for i, (s, v) in
             enumerate([(h_hbm, h), (dy_hbm, dy), (dyt_hbm, dyt), (ht_hbm, ht), (xt_hbm, ht)])]
    down = Reducer(grads[:10], True, t)
    up = Reducer(grads[10:], False, t)
    me = lax.axis_index('data')
    others = [{'data': lax.rem(me + k, OWN)} for k in range(1, OWN)]
    upper = t < NT
    lower = (t >= NT) & (t < TILES)

    @pl.when(t == 0)
    def _():
        for copy in loads[:4]:
            copy.start()
        neighbour_barrier(others + [down.peers['z']])
        acc[...] = jnp.zeros_like(acc)
        sq_down[...] = jnp.zeros_like(sq_down)
        sq_up[...] = jnp.zeros_like(sq_up)
        loads[0].wait()
        loads[1].wait()

    def upper_rows(first, last):
        wu = wu_ref[...]
        wd = wd_ref[0, :, 0].reshape(TILE, D)
        for r in range(first, last):
            if r < NB:
                rows = pl.ds(r * RM, RM)
                u_s[rows, :] = mm(h[rows, :], wu).astype(BF16)
                d_s[rows, :] = mm_nt(dy[rows, :], wd).astype(BF16)
            if r > 0:
                rows = pl.ds((r - 1) * RM, RM)
                u, slope = gelu_both(u_s[rows, :].astype(F32))
                dz = (d_s[rows, :].astype(F32) * slope).astype(BF16)
                u_s[rows, :] = u.astype(BF16)
                d_s[rows, :] = dz
                acc[rows, :] += mm_nt(dz, wu)

    def lower_rows(first, last):
        wd = wd_ref[0, :, 0].reshape(TILE, D)
        for r in range(first, last):
            if r < NB:
                rows = pl.ds(r * RM, RM)
                d_s[rows, :] = mm_nt(h[rows, :], wd).astype(BF16)
            if r > 0:
                rows = pl.ds((r - 1) * RM, RM)
                u, slope = gelu_both(z_ref[0, rows, :].astype(F32))
                u_s[rows, :] = u.astype(BF16)
                d_s[rows, :] = (d_s[rows, :].astype(F32) * slope).astype(BF16)

    def grads_early(rows):
        part_down[...] = mm(dyt[:, :rows], u_s[:rows, :])
        part_up[...] = mm(ht[:, :rows], d_s[:rows, :])

    def grads_late(rows):
        down.tile[...] = (part_down[...] + mm(dyt[:, rows:], u_s[rows:, :])).T.reshape(2, 2, 2, PIECE, D)
        up.tile[...] = (part_up[...] + mm(ht[:, rows:], d_s[rows:, :])).reshape(2, 2, 2, UP_ROWS, TILE)

    early = EARLY * RM

    @pl.when(upper)
    def _():
        upper_rows(0, EARLY + 1)

    @pl.when(lower)
    def _():
        lower_rows(0, EARLY + 1)

    down.progress(gd_ref, sq_down)

    @pl.when(t == 0)
    def _():
        loads[2].wait()
        loads[3].wait()

    @pl.when(t == NT)
    def _():
        loads[4].wait()

    @pl.when(upper)
    def _():
        upper_rows(EARLY + 1, NB)
        grads_early(early)

    @pl.when(lower)
    def _():
        lower_rows(EARLY + 1, NB)
        grads_early(early)

    up.progress(gu_ref, sq_up)

    @pl.when(upper)
    def _():
        upper_rows(NB, NB + 1)
        grads_late(early)

    @pl.when(lower)
    def _():
        lower_rows(NB, NB + 1)
        grads_late(early)

    @pl.when(t < TILES)
    def _():
        down.start()
        up.start()

    @pl.when(t == NT - 1)
    def _():
        loads[4].start()
        h[...] = acc[...].astype(BF16)
        dyt[...] = h[...].T

    @pl.when(t == GRID - 1)
    def _():
        part = jnp.sum(sq_down[...], axis=1, keepdims=True) + jnp.sum(sq_up[...], axis=1, keepdims=True)
        part = jnp.sum(part, axis=0, keepdims=True)
        sq_mine[...] = jnp.broadcast_to(part, sq_mine.shape)
        sq_all[me] = sq_mine[...]
        copies = [pltpu.make_async_remote_copy(
            src_ref=sq_mine, dst_ref=sq_all.at[me], send_sem=sq_send.at[k], recv_sem=sq_recv.at[k],
            device_id=others[k], device_id_type=MESH) for k in range(OWN - 1)]
        for copy in copies:
            copy.start()
        for copy in copies:
            copy.wait()
        total = sq_all[0]
        for k in range(1, OWN):
            total = total + sq_all[k]
        norm_ref[...] = total


def backward(h, ht, dy, dyt, xt, w_two, w_down5, z):
    anyspec = pl.BlockSpec(memory_space=pl.ANY)

    def final_tile(t):
        return jnp.clip(t - LAG, 0, TILES - 1)

    def layer_and_tile(t):
        first = t < NT
        return jnp.where(first, 1, 0), jnp.where(first, t, jnp.minimum(t - NT, NT - 1))

    def down_index(t):
        layer, tile = layer_and_tile(t)
        return layer, 0, tile, 0, 0

    return pl.pallas_call(
        backward_kernel,
        grid=(GRID,),
        in_specs=[anyspec] * 5 + [
            pl.BlockSpec((D, TILE), lambda t: (0, jnp.minimum(t, NT - 1))),
            pl.BlockSpec((1, OWN, 1, PIECE, D), down_index),
            pl.BlockSpec((1, ROWS, TILE), lambda t: (jnp.clip(t - NT, 0, NT - 1), 0, 0)),
        ],
        out_specs=[
            pl.BlockSpec((1, PIECE, D), lambda t: (final_tile(t), 0, 0)),
            pl.BlockSpec((1, UP_ROWS, TILE), lambda t: (final_tile(t), 0, 0)),
            pl.BlockSpec((8, 128), lambda t: (0, 0)),
        ],
        out_shape=[jax.ShapeDtypeStruct((TILES, PIECE, D), F32), jax.ShapeDtypeStruct((TILES, UP_ROWS, TILE), F32),
                   jax.ShapeDtypeStruct((8, 128), F32)],
        scratch_shapes=[pltpu.VMEM((ROWS, D), BF16), pltpu.VMEM((D, ROWS), BF16),
                        pltpu.VMEM((ROWS, D), BF16), pltpu.VMEM((D, ROWS), BF16),
                        pltpu.VMEM((ROWS, D), F32), pltpu.VMEM((ROWS, TILE), BF16), pltpu.VMEM((ROWS, TILE), BF16),
                        pltpu.VMEM((D, TILE), F32), pltpu.VMEM((D, TILE), F32),
                        pltpu.VMEM((8, D), F32), pltpu.VMEM((8, TILE), F32),
                        pltpu.SemaphoreType.DMA((5,)),
                        pltpu.VMEM((8, 128), F32), pltpu.VMEM((OWN, 8, 128), F32),
                        pltpu.SemaphoreType.DMA((OWN - 1,)), pltpu.SemaphoreType.DMA((OWN - 1,))]
        + grad_scratch(PIECE, D) + grad_scratch(UP_ROWS, TILE),
        compiler_params=pltpu.CompilerParams(vmem_limit_bytes=VMEM_LIMIT, collective_id=0, has_side_effects=True),
        name="backward",
    )(h, ht, dy, dyt, xt, w_two, w_down5, z)


def adam_update(grad_vals, master_vals, mom_vals, var_vals, clip_scale):
    new_mom = BETA1 * mom_vals + (1.0 - BETA1) * clip_scale * grad_vals
    new_var = BETA2 * var_vals + (1.0 - BETA2) * (clip_scale * clip_scale) * (grad_vals * grad_vals)
    new_master = master_vals - LEARN_RATE * (new_mom / BIAS_ONE) / (jnp.sqrt(new_var / BIAS_TWO) + ADAM_EPS)
    return new_master, new_mom, new_var


def norm_and_clip(sq_ref, clip_ref):
    norm = jnp.sqrt(sq_ref[...]) / DEVICES
    return norm, jnp.minimum(1.0, clip_ref[0, 0] / (norm + NORM_EPS))[0:1, 0:1]


def adam_up_kernel(sq_ref, clip_ref, g_ref, master_ref, mom_ref, var_ref,
                   new_w_ref, new_master_ref, new_mom_ref, new_var_ref):
    _, scale = norm_and_clip(sq_ref, clip_ref)
    for n in range(FF // 128):
        pieces = [divmod(4 * n + q, NT) for q in range(4)]
        grad = jnp.concatenate([g_ref[t, :, d * PIECE:(d + 1) * PIECE] for d, t in pieces], axis=1) / DEVICES
        cols = pl.ds(n * 128, 128)
        master, mom, var = adam_update(grad, master_ref[0, :, cols], mom_ref[0, :, cols], var_ref[0, :, cols], scale)
        new_master_ref[0, :, cols] = master
        new_mom_ref[0, :, cols] = mom
        new_var_ref[0, :, cols] = var
        new_w_ref[0, :, cols] = master.astype(BF16)


def adam_down_kernel(sq_ref, clip_ref, g_ref, master_ref, mom_ref, var_ref,
                     new_w_ref, new_master_ref, new_mom_ref, new_var_ref, norm_ref):
    norm, scale = norm_and_clip(sq_ref, clip_ref)
    norm_ref[...] = norm

    def body(i, carry):
        rows = pl.ds(pl.multiple_of(i * 16, 16), 16)
        master, mom, var = adam_update(g_ref[0, rows, :] / DEVICES, master_ref[0, rows, :], mom_ref[0, rows, :],
                                       var_ref[0, rows, :], scale)
        new_master_ref[0, rows, :] = master
        new_mom_ref[0, rows, :] = mom
        new_var_ref[0, rows, :] = var
        new_w_ref[0, rows, :] = master.astype(BF16)
        return carry

    lax.fori_loop(0, g_ref.shape[1] // 16, body, 0)


def adam_call(kernel, name, square_sum, clip, grad, g_spec, master, mom, var, block, with_norm):
    layers, rows, cols = master.shape
    state = pl.BlockSpec((1, block, cols), lambda layer, i: (layer, i, 0))
    small = pl.BlockSpec((8, 128), lambda layer, i: (0, 0))
    out_specs = [state] * 4 + ([small] if with_norm else [])
    out_shape = [jax.ShapeDtypeStruct(master.shape, BF16)] + [jax.ShapeDtypeStruct(master.shape, F32)] * 3
    if with_norm:
        out_shape = out_shape + [jax.ShapeDtypeStruct((8, 128), F32)]
    return pl.pallas_call(
        kernel,
        grid=(layers, rows // block),
        in_specs=[small, pl.BlockSpec(memory_space=pltpu.SMEM), g_spec, state, state, state],
        out_specs=out_specs,
        out_shape=out_shape,
        compiler_params=pltpu.CompilerParams(vmem_limit_bytes=VMEM_LIMIT),
        name=name,
    )(square_sum, clip, grad, master, mom, var)


UP_CHUNKS = [(True, 0, 16), (True, 16, 32), (True, 48, 32), (True, 80, 32)]
DOWN_CHUNKS = [(False, 0, 144), (False, 144, 144), (False, 288, 160), (False, 448, 160)]
CHUNKS = UP_CHUNKS + DOWN_CHUNKS
NC = len(CHUNKS)
GROUPS = 14


def gather_kernel(up_hbm, down_hbm, out_up, out_down, up_v, down_v, send, recv, local):
    d, c, x, y, z, peers = coordinates()
    d_x = d + 2 - 4 * x
    d_y = d + 4 - 8 * y
    d_xy = d_x + 4 - 8 * y
    other_core = 1 - 2 * c

    loads = [pltpu.make_async_copy(up_hbm, up_v, local.at[0]), pltpu.make_async_copy(down_hbm, down_v, local.at[1])]
    for copy in loads:
        copy.start()
    neighbour_barrier([peers[k] for k in 'cxyz'])
    for copy in loads:
        copy.wait()

    def region(chunk, layer, owner):
        is_up, first, count = CHUNKS[chunk]
        out, rows = (out_up, UP_ROWS) if is_up else (out_down, DOWN_ROWS)
        return out.at[layer, pl.ds(pl.multiple_of(owner * rows + first, 16), count)]

    def mine(chunk, layer):
        is_up, first, count = CHUNKS[chunk]
        return (up_v if is_up else down_v).at[layer, pl.ds(first, count)]

    started = []

    def send_chunk(group, chunk, src, layer, owner, peer):
        copy = pltpu.make_async_remote_copy(
            src_ref=src, dst_ref=region(chunk, layer, owner), send_sem=send.at[group, chunk],
            recv_sem=recv.at[group, chunk], device_id=peers[peer], device_id_type=MESH)
        copy.start()
        started.append(copy)

    def arrived(group, chunk, layer, owner):
        pltpu.make_async_remote_copy(
            src_ref=region(chunk, layer, owner), dst_ref=region(chunk, layer, owner), send_sem=send.at[group, chunk],
            recv_sem=recv.at[group, chunk], device_id=peers['c'], device_id_type=MESH).wait_recv()

    for k in range(NC):
        send_chunk(0, k, mine(k, z), z, d, 'x')
        send_chunk(1, k, mine(k, 1 - z), 1 - z, d, 'y')
    for k in range(NC):
        send_chunk(6, k, mine(k, 0), 0, d, 'c')
        send_chunk(7, k, mine(k, 1), 1, d, 'c')
    stores = []
    for layer in range(2):
        stores.append(pltpu.make_async_copy(up_v.at[layer], out_up.at[layer, pl.ds(pl.multiple_of(d * UP_ROWS, 16), UP_ROWS)], local.at[2 + layer]))
        stores.append(pltpu.make_async_copy(down_v.at[layer], out_down.at[layer, pl.ds(pl.multiple_of(d * DOWN_ROWS, 16), DOWN_ROWS)], local.at[4 + layer]))
    for copy in stores:
        copy.start()

    def second(k):
        for group, core_group, layer, owner in ((4, 10, 1 - z, d_x), (5, 11, z, d_y), (2, 12, z, d_xy), (3, 13, 1 - z, d_xy)):
            arrived(group, k, layer, owner)
            send_chunk(core_group, k, region(k, layer, owner), layer, owner, 'c')

    for k in range(NC):
        arrived(0, k, z, d_x)
        src = region(k, z, d_x)
        send_chunk(4, k, src, z, d_x, 'z')
        send_chunk(2, k, src, z, d_x, 'y')
        send_chunk(8, k, src, z, d_x, 'c')
        arrived(1, k, 1 - z, d_y)
        src = region(k, 1 - z, d_y)
        send_chunk(5, k, src, 1 - z, d_y, 'z')
        send_chunk(3, k, src, 1 - z, d_y, 'x')
        send_chunk(9, k, src, 1 - z, d_y, 'c')
    for k in range(NC):
        second(k)
    for k in range(NC):
        for group, layer, owner in ((6, 0, d), (7, 1, d), (8, z, d_x), (9, 1 - z, d_y), (10, 1 - z, d_x),
                                    (11, z, d_y), (12, z, d_xy), (13, 1 - z, d_xy)):
            arrived(group, k, layer, owner + other_core)
    for copy in started:
        copy.wait_send()
    for copy in stores:
        copy.wait()


def gather(up_shard, down_shard):
    anyspec = pl.BlockSpec(memory_space=pl.ANY)
    return pl.pallas_call(
        gather_kernel,
        in_specs=[anyspec, anyspec],
        out_specs=[anyspec, anyspec],
        out_shape=[jax.ShapeDtypeStruct((2, D, FF), BF16), jax.ShapeDtypeStruct((2, FF, D), BF16)],
        scratch_shapes=[pltpu.VMEM((2, UP_ROWS, FF), BF16), pltpu.VMEM((2, DOWN_ROWS, D), BF16),
                        pltpu.SemaphoreType.DMA((GROUPS, NC)), pltpu.SemaphoreType.DMA((GROUPS, NC)),
                        pltpu.SemaphoreType.DMA((6,))],
        compiler_params=pltpu.CompilerParams(vmem_limit_bytes=VMEM_LIMIT, collective_id=2, has_side_effects=True),
        name="gather",
    )(up_shard, down_shard)


def solution(mesh):
    batch_spec = P(('replica', 'data'), None)
    whole_spec = P()
    shard_spec = P(None, 'data', None)

    def device_step(inp_rows, out_grad, w_up, w_down, master_up, master_down, mom_up, mom_down, var_up, var_down, clip_norm):
        w_one = permute_first(w_up)
        w_down5 = w_down.reshape(2, OWN, NT, PIECE, D)
        pre_one, mid_rows, mid_t, inp_t, grad_t, w_two = forward(inp_rows, out_grad, w_one, w_down5, w_up)
        grad_down, grad_up, square_sum = backward(mid_rows, mid_t, out_grad, grad_t, inp_t, w_two, w_down5, pre_one)
        clip = clip_norm.reshape(1, 1)
        w_up_shard, master_up_new, mom_up_new, var_up_new = adam_call(
            adam_up_kernel, "adam_up", square_sum, clip, grad_up,
            pl.BlockSpec((NT, 16, TILE), lambda layer, i: (1 - layer, i, 0)), master_up, mom_up, var_up, 16, False)
        w_down_shard, master_down_new, mom_down_new, var_down_new, norm = adam_call(
            adam_down_kernel, "adam_down", square_sum, clip, grad_down.reshape(2, DOWN_ROWS, D),
            pl.BlockSpec((1, 304, D), lambda layer, i: (1 - layer, i, 0)), master_down, mom_down, var_down, 304, True)
        w_up_new, w_down_new = gather(w_up_shard, w_down_shard)
        return (w_up_new, w_down_new, master_up_new, master_down_new, mom_up_new, mom_down_new, var_up_new, var_down_new, norm[0, 0])

    return jax.shard_map(device_step, mesh=mesh, in_specs=(batch_spec, batch_spec, whole_spec, whole_spec, shard_spec, shard_spec, shard_spec, shard_spec, shard_spec, shard_spec, whole_spec), out_specs=(whole_spec, whole_spec, shard_spec, shard_spec, shard_spec, shard_spec, shard_spec, shard_spec, whole_spec), check_vma=False)
```

```python
import functools

import jax
import jax.numpy as jnp
from jax import lax
from jax.experimental import pallas as pl
from jax.experimental.pallas import tpu as pltpu
from jax.sharding import PartitionSpec as P

BETA1 = 0.9
BETA2 = 0.95
ADAM_EPS = 1e-8
LEARN_RATE = 5e-3
NORM_EPS = 1e-6
STEP = 10
BIAS_ONE = 1.0 - BETA1 ** STEP
BIAS_TWO = 1.0 - BETA2 ** STEP

F32 = jnp.float32
BF16 = jnp.bfloat16
ROWS = 4096
D = 896
FF = 4864
TILE = 256
NT = FF // TILE
OWN = 8
PIECE = TILE // OWN
UP_ROWS = D // OWN
DOWN_ROWS = FF // OWN
DEVICES = 16
RM = 256
NB = ROWS // RM
VMEM_LIMIT = 67_043_328


def gelu_value(pre_act):
    return pre_act * (0.5 + 0.5 * lax.erf(pre_act * 0.7071067811865476))


def gelu_both(pre_act):
    scaled = pre_act * 0.7071067811865476
    cdf = 0.5 + 0.5 * lax.erf(scaled)
    return pre_act * cdf, cdf + pre_act * jnp.exp2(scaled * scaled * -1.4426950408889634) * 0.3989422804014327


def mm(left, right):
    return jnp.dot(left, right, preferred_element_type=F32)


def mm_nt(left, right):
    return lax.dot_general(left, right, (((1,), (1,)), ((), ())), preferred_element_type=F32)


MESH = pl.DeviceIdType.MESH
LAG = 4
TILES = 2 * NT
GRID = TILES + LAG
EARLY = 12


def coordinates():
    d = lax.axis_index('data')
    z = lax.axis_index('replica')
    c = lax.rem(d, 2)
    x = lax.rem(lax.div(d, 2), 2)
    y = lax.div(d, 4)
    peers = {
        'c': {'data': d + 1 - 2 * c},
        'x': {'data': d + 2 - 4 * x},
        'y': {'data': d + 4 - 8 * y},
        'z': {'replica': 1 - z},
    }
    return d, c, x, y, z, peers


def neighbour_barrier(peers):
    barrier = pltpu.get_barrier_semaphore()
    for peer in peers:
        pl.semaphore_signal(barrier, inc=1, device_id=peer, device_id_type=MESH)
    pl.semaphore_wait(barrier, len(peers))


def grad_scratch(rows, cols):
    return [pltpu.VMEM((2, 2, 2, rows, cols), F32),
            pltpu.VMEM((2, 2, 2, rows, cols), F32),
            pltpu.VMEM((2, 2, rows, cols), F32),
            pltpu.VMEM((2, 2, rows, cols), F32),
            pltpu.VMEM((2, rows, cols), F32),
            pltpu.VMEM((2, rows, cols), F32),
            pltpu.VMEM((rows, cols), F32),
            pltpu.VMEM((2, rows, cols), F32),
            pltpu.SemaphoreType.DMA((4, 2)),
            pltpu.SemaphoreType.DMA((4, 2))]


class Reducer:
    def __init__(self, scratch, x_first, t):
        (self.tile, self.in_core, self.chip, self.in_one, self.two, self.in_two, self.four, self.in_rep,
         self.send, self.recv) = scratch
        self.x_first = x_first
        self.t = t
        _, self.c, self.x, self.y, _, self.peers = coordinates()

    def copy(self, stage, tile_index):
        slot = lax.rem(tile_index + 2, 2)
        first, second = ('x', 'y') if self.x_first else ('y', 'x')
        if stage == 0:
            src, dst, peer = self.tile.at[:, :, 1 - self.c], self.in_core.at[slot], 'c'
        elif stage == 1:
            src = self.chip.at[:, 1 - self.x] if self.x_first else self.chip.at[1 - self.y]
            dst, peer = self.in_one.at[slot], first
        elif stage == 2:
            src = self.two.at[1 - self.y] if self.x_first else self.two.at[1 - self.x]
            dst, peer = self.in_two.at[slot], second
        else:
            src, dst, peer = self.four, self.in_rep.at[slot], 'z'
        return pltpu.make_async_remote_copy(
            src_ref=src, dst_ref=dst, send_sem=self.send.at[stage, slot], recv_sem=self.recv.at[stage, slot],
            device_id=self.peers[peer], device_id_type=MESH)

    def start(self):
        self.copy(0, self.t).start()

    def progress(self, out_ref, sq_ref):
        t = self.t

        @pl.when(t >= 4)
        def _():
            self.copy(3, t - 4).wait()
            total = self.four[...] + self.in_rep[lax.rem(t, 2)]
            out_ref[0] = total
            sq_ref[...] += jnp.sum((total * total).reshape(-1, 8, total.shape[1]), axis=0)

        @pl.when((t >= 3) & (t < TILES + 3))
        def _():
            self.copy(2, t - 3).wait()
            mine = self.two[self.y] if self.x_first else self.two[self.x]
            self.four[...] = mine + self.in_two[lax.rem(t + 1, 2)]
            self.copy(3, t - 3).start()

        @pl.when((t >= 2) & (t < TILES + 2))
        def _():
            self.copy(1, t - 2).wait()
            mine = self.chip[:, self.x] if self.x_first else self.chip[self.y]
            self.two[...] = mine + self.in_one[lax.rem(t, 2)]
            self.copy(2, t - 2).start()

        @pl.when((t >= 1) & (t < TILES + 1))
        def _():
            self.copy(0, t - 1).wait()
            self.chip[...] = self.tile[:, :, self.c] + self.in_core[lax.rem(t + 1, 2)]
            self.copy(1, t - 1).start()


def permuted(w_ref, out_ref):
    for t in range(NT):
        out_ref[:, t * TILE:(t + 1) * TILE] = jnp.concatenate(
            [w_ref[0, :, d * DOWN_ROWS + t * PIECE:d * DOWN_ROWS + (t + 1) * PIECE] for d in range(OWN)], axis=1)


PERM_ROWS = 64


def permute_first(w_up):
    return pl.pallas_call(
        permuted,
        grid=(D // PERM_ROWS,),
        in_specs=[pl.BlockSpec((1, PERM_ROWS, FF), lambda i: (0, i, 0))],
        out_specs=pl.BlockSpec((PERM_ROWS, FF), lambda i: (i, 0)),
        out_shape=jax.ShapeDtypeStruct((D, FF), w_up.dtype),
        name="permute_first",
    )(w_up)


def forward_kernel(x_ref, dy_ref, wu_ref, wd_ref, next_ref, z_ref, h_ref, ht_ref, xt_ref, dyt_ref, next_out, acc):
    t = pl.program_id(0)
    block = jnp.minimum(t, ROWS // TILE - 1)

    @pl.when(t == 0)
    def _():
        acc[...] = jnp.zeros_like(acc)

    wd = wd_ref[0, :, 0].reshape(TILE, D)
    permuted(next_ref, next_out)
    for r in range(NB + 1):
        if r < NB:
            rows = pl.ds(r * RM, RM)
            z_ref[0, rows, :] = mm(x_ref[rows, :], wu_ref[...]).astype(BF16)
        if r > 0:
            rows = pl.ds((r - 1) * RM, RM)
            u = gelu_value(z_ref[0, rows, :].astype(F32)).astype(BF16)
            acc[rows, :] += mm(u, wd)
        if r == 2:
            xt_ref[...] = x_ref[pl.ds(pl.multiple_of(block * TILE, TILE), TILE), :].T
        if r == 5:
            dyt_ref[...] = dy_ref[...].T

    @pl.when(t == NT - 1)
    def _():
        h_ref[...] = acc[...].astype(BF16)
        ht_ref[...] = h_ref[...].T


def forward(x, dy, w_one, w_down5, w_up):
    last = ROWS // TILE - 1
    last_perm = D // PERM_ROWS - 1
    once = pl.Buffered(1)
    return pl.pallas_call(
        forward_kernel,
        grid=(NT,),
        in_specs=[
            pl.BlockSpec((ROWS, D), lambda t: (0, 0), pipeline_mode=once),
            pl.BlockSpec((TILE, D), lambda t: (jnp.minimum(t, last), 0)),
            pl.BlockSpec((D, TILE), lambda t: (0, t)),
            pl.BlockSpec((1, OWN, 1, PIECE, D), lambda t: (0, 0, t, 0, 0)),
            pl.BlockSpec((1, PERM_ROWS, FF), lambda t: (1, jnp.minimum(t, last_perm), 0)),
        ],
        out_specs=[
            pl.BlockSpec((1, ROWS, TILE), lambda t: (t, 0, 0)),
            pl.BlockSpec((ROWS, D), lambda t: (0, 0), pipeline_mode=once),
            pl.BlockSpec((D, ROWS), lambda t: (0, 0), pipeline_mode=once),
            pl.BlockSpec((D, TILE), lambda t: (0, jnp.minimum(t, last))),
            pl.BlockSpec((D, TILE), lambda t: (0, jnp.minimum(t, last))),
            pl.BlockSpec((PERM_ROWS, FF), lambda t: (jnp.minimum(t, last_perm), 0)),
        ],
        out_shape=[jax.ShapeDtypeStruct((NT, ROWS, TILE), BF16), jax.ShapeDtypeStruct((ROWS, D), BF16),
                   jax.ShapeDtypeStruct((D, ROWS), BF16), jax.ShapeDtypeStruct((D, ROWS), BF16),
                   jax.ShapeDtypeStruct((D, ROWS), BF16), jax.ShapeDtypeStruct((D, FF), BF16)],
        scratch_shapes=[pltpu.VMEM((ROWS, D), F32)],
        compiler_params=pltpu.CompilerParams(vmem_limit_bytes=VMEM_LIMIT),
        name="forward",
    )(x, dy, w_one, w_down5, w_up)


def backward_kernel(h_hbm, ht_hbm, dy_hbm, dyt_hbm, xt_hbm, wu_ref, wd_ref, z_ref, gd_ref, gu_ref, norm_ref,
                    h, ht, dy, dyt, acc, u_s, d_s, part_down, part_up, sq_down, sq_up, sems,
                    sq_mine, sq_all, sq_send, sq_recv, *grads):
    t = pl.program_id(0)
    loads = [pltpu.make_async_copy(s, v, sems.at[i]) for i, (s, v) in
             enumerate([(h_hbm, h), (dy_hbm, dy), (dyt_hbm, dyt), (ht_hbm, ht), (xt_hbm, ht)])]
    down = Reducer(grads[:10], True, t)
    up = Reducer(grads[10:], False, t)
    me = lax.axis_index('data')
    others = [{'data': lax.rem(me + k, OWN)} for k in range(1, OWN)]
    upper = t < NT
    lower = (t >= NT) & (t < TILES)

    @pl.when(t == 0)
    def _():
        for copy in loads[:4]:
            copy.start()
        neighbour_barrier(others + [down.peers['z']])
        acc[...] = jnp.zeros_like(acc)
        sq_down[...] = jnp.zeros_like(sq_down)
        sq_up[...] = jnp.zeros_like(sq_up)
        loads[0].wait()
        loads[1].wait()

    def upper_rows(first, last):
        wu = wu_ref[...]
        wd = wd_ref[0, :, 0].reshape(TILE, D)
        for r in range(first, last):
            if r < NB:
                rows = pl.ds(r * RM, RM)
                u_s[rows, :] = mm(h[rows, :], wu).astype(BF16)
                d_s[rows, :] = mm_nt(dy[rows, :], wd).astype(BF16)
            if r > 0:
                rows = pl.ds((r - 1) * RM, RM)
                u, slope = gelu_both(u_s[rows, :].astype(F32))
                dz = (d_s[rows, :].astype(F32) * slope).astype(BF16)
                u_s[rows, :] = u.astype(BF16)
                d_s[rows, :] = dz
                acc[rows, :] += mm_nt(dz, wu)

    def lower_rows(first, last):
        wd = wd_ref[0, :, 0].reshape(TILE, D)
        for r in range(first, last):
            if r < NB:
                rows = pl.ds(r * RM, RM)
                d_s[rows, :] = mm_nt(h[rows, :], wd).astype(BF16)
            if r > 0:
                rows = pl.ds((r - 1) * RM, RM)
                u, slope = gelu_both(z_ref[0, rows, :].astype(F32))
                u_s[rows, :] = u.astype(BF16)
                d_s[rows, :] = (d_s[rows, :].astype(F32) * slope).astype(BF16)

    def grads_early(rows):
        part_down[...] = mm(dyt[:, :rows], u_s[:rows, :])
        part_up[...] = mm(ht[:, :rows], d_s[:rows, :])

    def grads_late(rows):
        down.tile[...] = (part_down[...] + mm(dyt[:, rows:], u_s[rows:, :])).T.reshape(2, 2, 2, PIECE, D)
        up.tile[...] = (part_up[...] + mm(ht[:, rows:], d_s[rows:, :])).reshape(2, 2, 2, UP_ROWS, TILE)

    early = EARLY * RM

    @pl.when(upper)
    def _():
        upper_rows(0, EARLY + 1)

    @pl.when(lower)
    def _():
        lower_rows(0, EARLY + 1)

    down.progress(gd_ref, sq_down)

    @pl.when(t == 0)
    def _():
        loads[2].wait()
        loads[3].wait()

    @pl.when(t == NT)
    def _():
        loads[4].wait()

    @pl.when(upper)
    def _():
        upper_rows(EARLY + 1, NB)
        grads_early(early)

    @pl.when(lower)
    def _():
        lower_rows(EARLY + 1, NB)
        grads_early(early)

    up.progress(gu_ref, sq_up)

    @pl.when(upper)
    def _():
        upper_rows(NB, NB + 1)
        grads_late(early)

    @pl.when(lower)
    def _():
        lower_rows(NB, NB + 1)
        grads_late(early)

    @pl.when(t < TILES)
    def _():
        down.start()
        up.start()

    @pl.when(t == NT - 1)
    def _():
        loads[4].start()
        h[...] = acc[...].astype(BF16)
        dyt[...] = h[...].T

    @pl.when(t == GRID - 1)
    def _():
        part = jnp.sum(sq_down[...], axis=1, keepdims=True) + jnp.sum(sq_up[...], axis=1, keepdims=True)
        part = jnp.sum(part, axis=0, keepdims=True)
        sq_mine[...] = jnp.broadcast_to(part, sq_mine.shape)
        sq_all[me] = sq_mine[...]
        copies = [pltpu.make_async_remote_copy(
            src_ref=sq_mine, dst_ref=sq_all.at[me], send_sem=sq_send.at[k], recv_sem=sq_recv.at[k],
            device_id=others[k], device_id_type=MESH) for k in range(OWN - 1)]
        for copy in copies:
            copy.start()
        for copy in copies:
            copy.wait()
        total = sq_all[0]
        for k in range(1, OWN):
            total = total + sq_all[k]
        norm_ref[...] = total


def backward(h, ht, dy, dyt, xt, w_two, w_down5, z):
    anyspec = pl.BlockSpec(memory_space=pl.ANY)

    def final_tile(t):
        return jnp.clip(t - LAG, 0, TILES - 1)

    def layer_and_tile(t):
        first = t < NT
        return jnp.where(first, 1, 0), jnp.where(first, t, jnp.minimum(t - NT, NT - 1))

    def down_index(t):
        layer, tile = layer_and_tile(t)
        return layer, 0, tile, 0, 0

    return pl.pallas_call(
        backward_kernel,
        grid=(GRID,),
        in_specs=[anyspec] * 5 + [
            pl.BlockSpec((D, TILE), lambda t: (0, jnp.minimum(t, NT - 1))),
            pl.BlockSpec((1, OWN, 1, PIECE, D), down_index),
            pl.BlockSpec((1, ROWS, TILE), lambda t: (jnp.clip(t - NT, 0, NT - 1), 0, 0)),
        ],
        out_specs=[
            pl.BlockSpec((1, PIECE, D), lambda t: (final_tile(t), 0, 0)),
            pl.BlockSpec((1, UP_ROWS, TILE), lambda t: (final_tile(t), 0, 0)),
            pl.BlockSpec((8, 128), lambda t: (0, 0)),
        ],
        out_shape=[jax.ShapeDtypeStruct((TILES, PIECE, D), F32), jax.ShapeDtypeStruct((TILES, UP_ROWS, TILE), F32),
                   jax.ShapeDtypeStruct((8, 128), F32)],
        scratch_shapes=[pltpu.VMEM((ROWS, D), BF16), pltpu.VMEM((D, ROWS), BF16),
                        pltpu.VMEM((ROWS, D), BF16), pltpu.VMEM((D, ROWS), BF16),
                        pltpu.VMEM((ROWS, D), F32), pltpu.VMEM((ROWS, TILE), BF16), pltpu.VMEM((ROWS, TILE), BF16),
                        pltpu.VMEM((D, TILE), F32), pltpu.VMEM((D, TILE), F32),
                        pltpu.VMEM((8, D), F32), pltpu.VMEM((8, TILE), F32),
                        pltpu.SemaphoreType.DMA((5,)),
                        pltpu.VMEM((8, 128), F32), pltpu.VMEM((OWN, 8, 128), F32),
                        pltpu.SemaphoreType.DMA((OWN - 1,)), pltpu.SemaphoreType.DMA((OWN - 1,))]
        + grad_scratch(PIECE, D) + grad_scratch(UP_ROWS, TILE),
        compiler_params=pltpu.CompilerParams(vmem_limit_bytes=VMEM_LIMIT, collective_id=0, has_side_effects=True),
        name="backward",
    )(h, ht, dy, dyt, xt, w_two, w_down5, z)


def adam_update(grad_vals, master_vals, mom_vals, var_vals, clip_scale):
    new_mom = BETA1 * mom_vals + (1.0 - BETA1) * clip_scale * grad_vals
    new_var = BETA2 * var_vals + (1.0 - BETA2) * (clip_scale * clip_scale) * (grad_vals * grad_vals)
    new_master = master_vals - (LEARN_RATE / BIAS_ONE) * new_mom / (jnp.sqrt(new_var * (1.0 / BIAS_TWO)) + ADAM_EPS)
    return new_master, new_mom, new_var


def norm_and_clip(sq_ref, clip_ref):
    norm = jnp.sqrt(sq_ref[...]) / DEVICES
    return norm, jnp.minimum(1.0, clip_ref[0, 0] / (norm + NORM_EPS))[0:1, 0:1]


def adam_up_kernel(sq_ref, clip_ref, g_ref, master_ref, mom_ref, var_ref,
                   new_w_ref, new_master_ref, new_mom_ref, new_var_ref):
    _, scale = norm_and_clip(sq_ref, clip_ref)
    for n in range(FF // 128):
        pieces = [divmod(4 * n + q, NT) for q in range(4)]
        grad = jnp.concatenate([g_ref[t, :, d * PIECE:(d + 1) * PIECE] for d, t in pieces], axis=1) * (1.0 / DEVICES)
        cols = pl.ds(n * 128, 128)
        master, mom, var = adam_update(grad, master_ref[0, :, cols], mom_ref[0, :, cols], var_ref[0, :, cols], scale)
        new_master_ref[0, :, cols] = master
        new_mom_ref[0, :, cols] = mom
        new_var_ref[0, :, cols] = var
        new_w_ref[0, :, cols] = master.astype(BF16)


def adam_down_kernel(sq_ref, clip_ref, g_ref, master_ref, mom_ref, var_ref,
                     new_w_ref, new_master_ref, new_mom_ref, new_var_ref, norm_ref):
    norm, scale = norm_and_clip(sq_ref, clip_ref)
    norm_ref[...] = norm

    def body(i, carry):
        rows = pl.ds(pl.multiple_of(i * 16, 16), 16)
        master, mom, var = adam_update(g_ref[0, rows, :] * (1.0 / DEVICES), master_ref[0, rows, :], mom_ref[0, rows, :],
                                       var_ref[0, rows, :], scale)
        new_master_ref[0, rows, :] = master
        new_mom_ref[0, rows, :] = mom
        new_var_ref[0, rows, :] = var
        new_w_ref[0, rows, :] = master.astype(BF16)
        return carry

    lax.fori_loop(0, g_ref.shape[1] // 16, body, 0)


def adam_call(kernel, name, square_sum, clip, grad, g_spec, master, mom, var, block, with_norm):
    layers, rows, cols = master.shape
    state = pl.BlockSpec((1, block, cols), lambda layer, i: (layer, i, 0))
    small = pl.BlockSpec((8, 128), lambda layer, i: (0, 0))
    out_specs = [state] * 4 + ([small] if with_norm else [])
    out_shape = [jax.ShapeDtypeStruct(master.shape, BF16)] + [jax.ShapeDtypeStruct(master.shape, F32)] * 3
    if with_norm:
        out_shape = out_shape + [jax.ShapeDtypeStruct((8, 128), F32)]
    return pl.pallas_call(
        kernel,
        grid=(layers, rows // block),
        in_specs=[small, pl.BlockSpec(memory_space=pltpu.SMEM), g_spec, state, state, state],
        out_specs=out_specs,
        out_shape=out_shape,
        compiler_params=pltpu.CompilerParams(vmem_limit_bytes=VMEM_LIMIT),
        name=name,
    )(square_sum, clip, grad, master, mom, var)


UP_CHUNKS = [(True, 0, 16), (True, 16, 32), (True, 48, 32), (True, 80, 32)]
DOWN_CHUNKS = [(False, 0, 144), (False, 144, 144), (False, 288, 160), (False, 448, 160)]
CHUNKS = UP_CHUNKS + DOWN_CHUNKS
NC = len(CHUNKS)
GROUPS = 14


def gather_kernel(up_hbm, down_hbm, out_up, out_down, up_v, down_v, send, recv, local):
    d, c, x, y, z, peers = coordinates()
    d_x = d + 2 - 4 * x
    d_y = d + 4 - 8 * y
    d_xy = d_x + 4 - 8 * y
    other_core = 1 - 2 * c

    loads = [pltpu.make_async_copy(up_hbm, up_v, local.at[0]), pltpu.make_async_copy(down_hbm, down_v, local.at[1])]
    for copy in loads:
        copy.start()
    neighbour_barrier([peers[k] for k in 'cxyz'])
    for copy in loads:
        copy.wait()

    def region(chunk, layer, owner):
        is_up, first, count = CHUNKS[chunk]
        out, rows = (out_up, UP_ROWS) if is_up else (out_down, DOWN_ROWS)
        return out.at[layer, pl.ds(pl.multiple_of(owner * rows + first, 16), count)]

    def mine(chunk, layer):
        is_up, first, count = CHUNKS[chunk]
        return (up_v if is_up else down_v).at[layer, pl.ds(first, count)]

    started = []

    def send_chunk(group, chunk, src, layer, owner, peer):
        copy = pltpu.make_async_remote_copy(
            src_ref=src, dst_ref=region(chunk, layer, owner), send_sem=send.at[group, chunk],
            recv_sem=recv.at[group, chunk], device_id=peers[peer], device_id_type=MESH)
        copy.start()
        started.append(copy)

    def arrived(group, chunk, layer, owner):
        pltpu.make_async_remote_copy(
            src_ref=region(chunk, layer, owner), dst_ref=region(chunk, layer, owner), send_sem=send.at[group, chunk],
            recv_sem=recv.at[group, chunk], device_id=peers['c'], device_id_type=MESH).wait_recv()

    for k in range(NC):
        send_chunk(0, k, mine(k, z), z, d, 'x')
        send_chunk(1, k, mine(k, 1 - z), 1 - z, d, 'y')
    for k in range(NC):
        send_chunk(6, k, mine(k, 0), 0, d, 'c')
        send_chunk(7, k, mine(k, 1), 1, d, 'c')
    stores = []
    for layer in range(2):
        stores.append(pltpu.make_async_copy(up_v.at[layer], out_up.at[layer, pl.ds(pl.multiple_of(d * UP_ROWS, 16), UP_ROWS)], local.at[2 + layer]))
        stores.append(pltpu.make_async_copy(down_v.at[layer], out_down.at[layer, pl.ds(pl.multiple_of(d * DOWN_ROWS, 16), DOWN_ROWS)], local.at[4 + layer]))
    for copy in stores:
        copy.start()

    def second(k):
        for group, core_group, layer, owner in ((4, 10, 1 - z, d_x), (5, 11, z, d_y), (2, 12, z, d_xy), (3, 13, 1 - z, d_xy)):
            arrived(group, k, layer, owner)
            send_chunk(core_group, k, region(k, layer, owner), layer, owner, 'c')

    for k in range(NC):
        arrived(0, k, z, d_x)
        src = region(k, z, d_x)
        send_chunk(4, k, src, z, d_x, 'z')
        send_chunk(2, k, src, z, d_x, 'y')
        send_chunk(8, k, src, z, d_x, 'c')
        arrived(1, k, 1 - z, d_y)
        src = region(k, 1 - z, d_y)
        send_chunk(5, k, src, 1 - z, d_y, 'z')
        send_chunk(3, k, src, 1 - z, d_y, 'x')
        send_chunk(9, k, src, 1 - z, d_y, 'c')
    for k in range(NC):
        second(k)
    for k in range(NC):
        for group, layer, owner in ((6, 0, d), (7, 1, d), (8, z, d_x), (9, 1 - z, d_y), (10, 1 - z, d_x),
                                    (11, z, d_y), (12, z, d_xy), (13, 1 - z, d_xy)):
            arrived(group, k, layer, owner + other_core)
    for copy in started:
        copy.wait_send()
    for copy in stores:
        copy.wait()


def gather(up_shard, down_shard):
    anyspec = pl.BlockSpec(memory_space=pl.ANY)
    return pl.pallas_call(
        gather_kernel,
        in_specs=[anyspec, anyspec],
        out_specs=[anyspec, anyspec],
        out_shape=[jax.ShapeDtypeStruct((2, D, FF), BF16), jax.ShapeDtypeStruct((2, FF, D), BF16)],
        scratch_shapes=[pltpu.VMEM((2, UP_ROWS, FF), BF16), pltpu.VMEM((2, DOWN_ROWS, D), BF16),
                        pltpu.SemaphoreType.DMA((GROUPS, NC)), pltpu.SemaphoreType.DMA((GROUPS, NC)),
                        pltpu.SemaphoreType.DMA((6,))],
        compiler_params=pltpu.CompilerParams(vmem_limit_bytes=VMEM_LIMIT, collective_id=2, has_side_effects=True),
        name="gather",
    )(up_shard, down_shard)


def solution(mesh):
    batch_spec = P(('replica', 'data'), None)
    whole_spec = P()
    shard_spec = P(None, 'data', None)

    def device_step(inp_rows, out_grad, w_up, w_down, master_up, master_down, mom_up, mom_down, var_up, var_down, clip_norm):
        w_one = permute_first(w_up)
        w_down5 = w_down.reshape(2, OWN, NT, PIECE, D)
        pre_one, mid_rows, mid_t, inp_t, grad_t, w_two = forward(inp_rows, out_grad, w_one, w_down5, w_up)
        grad_down, grad_up, square_sum = backward(mid_rows, mid_t, out_grad, grad_t, inp_t, w_two, w_down5, pre_one)
        clip = clip_norm.reshape(1, 1)
        w_up_shard, master_up_new, mom_up_new, var_up_new = adam_call(
            adam_up_kernel, "adam_up", square_sum, clip, grad_up,
            pl.BlockSpec((NT, 16, TILE), lambda layer, i: (1 - layer, i, 0)), master_up, mom_up, var_up, 16, False)
        w_down_shard, master_down_new, mom_down_new, var_down_new, norm = adam_call(
            adam_down_kernel, "adam_down", square_sum, clip, grad_down.reshape(2, DOWN_ROWS, D),
            pl.BlockSpec((1, 304, D), lambda layer, i: (1 - layer, i, 0)), master_down, mom_down, var_down, 304, True)
        w_up_new, w_down_new = gather(w_up_shard, w_down_shard)
        return (w_up_new, w_down_new, master_up_new, master_down_new, mom_up_new, mom_down_new, var_up_new, var_down_new, norm[0, 0])

    return jax.shard_map(device_step, mesh=mesh, in_specs=(batch_spec, batch_spec, whole_spec, whole_spec, shard_spec, shard_spec, shard_spec, shard_spec, shard_spec, shard_spec, whole_spec), out_specs=(whole_spec, whole_spec, shard_spec, shard_spec, shard_spec, shard_spec, shard_spec, shard_spec, whole_spec), check_vma=False)
```
